128 devices in a mesh: gx: 8 (over z, core), gy: 16 (over x, y).
Axes of the slice: x: 4, y: 4, z: 4, core: 2. Of those that a mesh axis runs over, the one named last changes fastest.
Arguments:
- atm_members: float32 [8, 16, 80, 12, 128], P('gx', 'gy'), may hold values from -6 to 6
- ocean_members: bfloat16 [8, 16, 80, 1024], P('gx', 'gy'), may hold values from -6 to 6
- remap_weights: bfloat16 [8, 16, 4, 1024, 128], P('gx', 'gy'), may hold values from -0.09375 to 0.09375
- pair_src: int32 [8, 16, 4], P('gx', 'gy'), may hold values from 0 to 127, as said below
- obs_cell: int32 [8, 16, 64], P('gx', 'gy'), may hold values from 0 to 127
- obs_value: float32 [8, 16, 64], P('gx', 'gy'), may hold values from -8 to 8
- obs_error: float32 [8, 16, 64], P('gx', 'gy'), may hold values from 2 to 16
- obs_live: int32 [8, 16, 64], P('gx', 'gy'), may hold values from 0 to 1, as said below
- obs_order: int32 [8, 16, 64], P('gx', 'gy'), may hold values from 0 to 63, each once within a row
Outputs:
- post_mean: float32 [8, 16, 13, 128], P('gx', 'gy')
- post_anom: float32 [8, 16, 80, 13, 128], P('gx', 'gy')
The draws below stay inside these ranges and needn't reach their ends.
Inputs may be any that keep to these rules, and one draw needn't show every extreme that they name: `pair_src`: for atmosphere tile (i, j) the 4 numbers are distinct, each a * 16 + b with |a - i| <= 1 and |b - j| <= 1. `obs_live`: the live slots of a tile are its first ones, between 8 and 64 of them; some tile has all slots live. `obs_order`: each tile's last dimension is a permutation of its slots.
All inputs are finite; a program needn't handle non-finite values.
Results may differ from the reference program's by a relative error of at most 0.0003.
Values may be sent and summed in bfloat16 or wider, within the bound.
No kernel may reach another device: no remote copies, remote signals or barrier semaphores. Data moves between devices by JAX's collectives and lax.ppermute only.
A program may use at most 64 MiB of HBM per device.

```python
import math
import jax
import jax.numpy as jnp
from jax import lax

MEM = 80
AX = 8
AY = 16
OCN_DEV = 1024
OB = 32
NB = 2
K = 4
FIELDS = 12
COMP = 13
CELLS = 128
RAD = 2
OBS_DEV = 64
TILES_X = 8
TILES_Y = 16


def draw_pair_src(key, part):
    tile_x = jnp.arange(TILES_X, dtype=jnp.int32)[:, None, None]
    tile_y = jnp.arange(TILES_Y, dtype=jnp.int32)[None, :, None]
    candidate = jnp.arange(9, dtype=jnp.int32)[None, None, :]
    source_x = tile_x + candidate // 3 - 1
    source_y = tile_y + candidate % 3 - 1
    scores = jax.random.randint(jax.random.fold_in(key, 11), (TILES_X, TILES_Y, 9), 0, 1 << 20)
    scores = scores * 9 + candidate
    outside = (source_x < 0) | (source_x >= TILES_X) | (source_y < 0) | (source_y >= TILES_Y)
    scores = jnp.where(outside, scores + (1 << 29), scores)
    ranking = jnp.argsort(scores, axis=-1)[..., :K]
    linear = source_x * TILES_Y + source_y
    return jnp.take_along_axis(linear, ranking, axis=-1).astype(jnp.int32)


def draw_obs_live(key, part):
    threshold = jax.random.randint(jax.random.fold_in(key, 21), (TILES_X, TILES_Y), OBS_DEV // 8, OBS_DEV + 1)
    chosen_tile = jax.random.randint(jax.random.fold_in(key, 22), (), 0, TILES_X * TILES_Y)
    tile_number = jnp.arange(TILES_X * TILES_Y, dtype=jnp.int32).reshape(TILES_X, TILES_Y)
    threshold = jnp.where(tile_number == chosen_tile, OBS_DEV, threshold)
    slot_number = jnp.arange(OBS_DEV, dtype=jnp.int32)
    return (slot_number[None, None, :] < threshold[:, :, None]).astype(jnp.int32)


def plant(values, rng, smallest, top_value):
    longest = values.shape.index(max(values.shape))
    spots = []
    for shift in (0, 1):
        where = [jax.random.randint(jax.random.fold_in(rng, axis), (), 0, length) for axis, length in enumerate(values.shape)]
        where[longest] = (where[longest] + shift) % values.shape[longest]
        spots.append(tuple(where))
    return values.at[spots[0]].set(smallest).at[spots[1]].set(top_value)


def levels(key, shape, pieces, smallest, high):
    level, own = 1.0, jax.random.fold_in(key, 6)
    for axis_at, shards_of in pieces:
        heights = jnp.exp(jax.random.uniform(jax.random.fold_in(own, axis_at), (shards_of,), jnp.float32, smallest / len(pieces), high / len(pieces)))
        level = level * jnp.repeat(heights, shape[axis_at] // shards_of).reshape([-1 if axis == axis_at else 1 for axis in range(len(shape))])
    return level


def centred(rng, shape, spread, limit, pieces=(), held_as=jnp.bfloat16):
    values = spread * jax.random.normal(rng, shape, jnp.float32)
    if pieces:
        values = values * levels(rng, shape, pieces, -0.22, 0.18)
    return jnp.clip(values, -limit, limit).astype(held_as)


def setup_inputs(seed: int = 0) -> dict:
    splits = jax.random.split(jax.random.key(seed), 10)
    atm_members = centred(splits[0], (TILES_X, TILES_Y, MEM, FIELDS, CELLS), 1.0, 6.0, ((0, 8), (1, 16)), jnp.float32)
    ocean_members = centred(splits[1], (TILES_X, TILES_Y, MEM, OCN_DEV), 1.0, 6.0, ((0, 8), (1, 16)))
    remap_weights = centred(splits[2], (TILES_X, TILES_Y, K, OCN_DEV, CELLS), (K * OCN_DEV) ** -0.5, 0.09375, ((0, 8), (1, 16)))
    pair_src = draw_pair_src(jax.random.fold_in(splits[9], 71), 0)
    obs_cell = plant(jax.random.randint(splits[4], (TILES_X, TILES_Y, OBS_DEV), 0, CELLS), jax.random.fold_in(splits[4], 1), 0, CELLS - 1).astype(jnp.int32)
    obs_value = centred(splits[5], (TILES_X, TILES_Y, OBS_DEV), 1.5, 8.0, ((0, 8), (1, 16)), jnp.float32)
    obs_error = jnp.clip(jnp.exp(math.log(16.0) - 2.0794415 * jax.random.uniform(splits[6], (TILES_X, TILES_Y, OBS_DEV), jnp.float32) ** levels(splits[6], (TILES_X, TILES_Y, OBS_DEV), ((0, 8), (1, 16)), -0.2, 0.2)), 2.0, 16.0)
    obs_live = draw_obs_live(jax.random.fold_in(splits[9], 71), 0)
    obs_order = jax.vmap(lambda own: jax.random.permutation(own, OBS_DEV))(jax.random.split(splits[8], TILES_X * TILES_Y)).reshape((TILES_X, TILES_Y, OBS_DEV)).astype(jnp.int32)
    return {"atm_members": atm_members, "ocean_members": ocean_members, "remap_weights": remap_weights, "pair_src": pair_src, "obs_cell": obs_cell, "obs_value": obs_value, "obs_error": obs_error, "obs_live": obs_live, "obs_order": obs_order}


exact_mode = lax.Precision.HIGHEST

def update_group(packets, anomaly, ens_mean, base_x, base_y):
    members = anomaly.shape[0]
    components = anomaly.shape[1]
    cell_count = anomaly.shape[2]
    observed = jnp.transpose(packets[:, :members, :], (1, 0, 2)).reshape(members, -1)
    innovation = packets[:, members, :].reshape(-1)
    errors = packets[:, members + 1, :].reshape(-1)
    obs_x = packets[:, members + 2, :].reshape(-1)
    obs_y = packets[:, members + 3, :].reshape(-1)
    live = packets[:, members + 4, :].reshape(-1)
    variance = lax.optimization_barrier(jnp.sum(observed * observed, axis=0)) / (members - 1)
    denominator = variance + errors + (1.0 - live)
    weighting = live / denominator
    damping = 1.0 / (1.0 + jnp.sqrt(errors / denominator))
    cell_index = jnp.arange(cell_count, dtype=jnp.int32)
    cell_x = (base_x + cell_index // AY).astype(jnp.float32)
    cell_y = (base_y + cell_index % AY).astype(jnp.float32)
    distance = (obs_x[:, None] - cell_x[None, :]) ** 2 + (obs_y[:, None] - cell_y[None, :]) ** 2
    taper = jnp.maximum(1.0 - distance / float(RAD * RAD), 0.0) ** 2
    flat_anomaly = anomaly.reshape(members, components * cell_count)
    covariance = jnp.dot(observed.T, flat_anomaly, precision=exact_mode, preferred_element_type=jnp.float32) / (members - 1)
    gain = covariance.reshape(-1, components, cell_count) * (taper * weighting[:, None])[:, None, :]
    gain = gain.reshape(-1, components * cell_count)
    mean_step = jnp.dot(innovation[None, :], gain, precision=exact_mode, preferred_element_type=jnp.float32)
    anomaly_step = jnp.dot(observed * damping[None, :], gain, precision=exact_mode, preferred_element_type=jnp.float32)
    return (mean_step.reshape(components, cell_count), anomaly_step.reshape(members, components, cell_count))

def reference(atm_members, ocean_members, remap_weights, pair_src, obs_cell, obs_value, obs_error, obs_live, obs_order):
    tiles = TILES_X * TILES_Y
    ocean_flat = ocean_members.reshape(tiles, MEM, OCN_DEV)

    def remap_one(inputs):
        weights, sources = inputs
        chosen = ocean_flat[sources]
        stacked = jnp.transpose(chosen, (1, 0, 2)).reshape(MEM, K * OCN_DEV)
        return jnp.dot(stacked, weights.reshape(K * OCN_DEV, CELLS), preferred_element_type=jnp.float32)
    surface = lax.map(remap_one, (remap_weights.reshape(tiles, K, OCN_DEV, CELLS), pair_src.reshape(tiles, K).astype(jnp.int32)))
    state = jnp.concatenate([atm_members.reshape(tiles, MEM, FIELDS, CELLS), surface[:, :, None, :]], axis=2)
    ens_mean = lax.optimization_barrier(jnp.sum(state, axis=1)) / MEM
    anomaly = state - ens_mean[:, None]
    ens_mean = ens_mean.reshape(TILES_X, TILES_Y, COMP, CELLS)
    anomaly = anomaly.reshape(TILES_X, TILES_Y, MEM, COMP, CELLS)
    tile_x = jnp.broadcast_to(jnp.arange(TILES_X, dtype=jnp.int32)[:, None], (TILES_X, TILES_Y))
    tile_y = jnp.broadcast_to(jnp.arange(TILES_Y, dtype=jnp.int32)[None, :], (TILES_X, TILES_Y))
    base_x = tile_x * AX
    base_y = tile_y * AY
    for batch_index in range(NB):
        obs_slots = obs_order[:, :, batch_index * OB:(batch_index + 1) * OB].astype(jnp.int32)
        obs_cells = jnp.take_along_axis(obs_cell.astype(jnp.int32), obs_slots, axis=2)
        values = jnp.take_along_axis(obs_value, obs_slots, axis=2)
        errors = jnp.take_along_axis(obs_error, obs_slots, axis=2)
        live = jnp.take_along_axis(obs_live, obs_slots, axis=2).astype(jnp.float32)
        observed = jnp.take_along_axis(anomaly[:, :, :, FIELDS, :], obs_cells[:, :, None, :], axis=3)
        predicted = jnp.take_along_axis(ens_mean[:, :, FIELDS, :], obs_cells, axis=2)
        pos_x = (base_x[:, :, None] + obs_cells // AY).astype(jnp.float32)
        pos_y = (base_y[:, :, None] + obs_cells % AY).astype(jnp.float32)
        extras = jnp.stack([values - predicted, errors, pos_x, pos_y, live], axis=2)
        packet = jnp.concatenate([observed, extras], axis=2)
        padded = jnp.pad(packet, ((1, 1), (1, 1), (0, 0), (0, 0)))
        beside_all = jnp.stack([padded[row_shift:row_shift + TILES_X, col_shift:col_shift + TILES_Y] for row_shift in range(3) for col_shift in range(3)], axis=2)

        def one_tile(inputs):
            packets, tile_anomaly, tile_mean, anchor_x, anchor_y = inputs
            mean_step, anomaly_step = update_group(packets, tile_anomaly, tile_mean, anchor_x, anchor_y)
            return (tile_mean + mean_step, tile_anomaly - anomaly_step)
        new_mean, new_anomaly = lax.map(one_tile, (beside_all.reshape(tiles, 9, MEM + 5, OB), anomaly.reshape(tiles, MEM, COMP, CELLS), ens_mean.reshape(tiles, COMP, CELLS), base_x.reshape(tiles), base_y.reshape(tiles)))
        ens_mean = new_mean.reshape(TILES_X, TILES_Y, COMP, CELLS)
        anomaly = new_anomaly.reshape(TILES_X, TILES_Y, MEM, COMP, CELLS)
    return (ens_mean, anomaly)
```

```python
import functools

import jax
import jax.numpy as jnp
from jax import lax
from jax.experimental import pallas as pl
from jax.experimental.pallas import tpu as pltpu
from jax.sharding import PartitionSpec as P

MEM = 80
AX = 8
AY = 16
OCN_DEV = 1024
OB = 32
NB = 2
K = 4
FIELDS = 12
COMP = 13
CELLS = 128
OBS_DEV = 64

f32 = jnp.float32
META = 4
TAPER = {0: 1.0, 1: 0.5625, 2: 0.25}
OFFSETS = [(dx, dy) for dx in (-1, 0, 1) for dy in (-1, 0, 1)]


def ring(block, axis, step):
    count = lax.axis_size(axis)
    return lax.ppermute(block, axis, [(i, (i + step) % count) for i in range(count)])


def swap(block, axis, first):
    count = lax.axis_size(axis)
    pairs = []
    for at in range(first, count + first, 2):
        low, high = at % count, (at + 1) % count
        pairs += [(low, high), (high, low)]
    return lax.ppermute(block, axis, sorted(pairs))


def lanes(rows=1):
    return lax.broadcasted_iota(jnp.int32, (rows, CELLS), 1)


def remap_kernel(sel_ref, meta_ref, w_ref, *refs):
    tiles, (state_ref, message_ref) = refs[:9], refs[9:]
    state_ref[...] = jnp.zeros_like(state_ref)

    def one(k, carry):
        for index, tile in enumerate(tiles):

            @pl.when(sel_ref[k] == index)
            def _():
                state_ref[...] += jnp.dot(tile[...], w_ref[k], preferred_element_type=f32)

        return carry

    lax.fori_loop(0, K, one, 0)
    lane = lanes()
    message_ref[...] = jnp.where(
        (lane >= META) & (lane < META + 3), meta_ref[...], state_ref[...]
    )


def anomaly_kernel(atm_ref, state_ref, mean_ref, anom_ref):
    total = jnp.sum(atm_ref[...], axis=0) / MEM
    surface = state_ref[...]
    sst_mean = jnp.sum(surface, axis=0, keepdims=True) / MEM
    mean_ref[...] = jnp.zeros_like(mean_ref)
    mean_ref[0:FIELDS, :] = total
    mean_ref[FIELDS : FIELDS + 1, :] = sst_mean

    def one(m, carry):
        anom_ref[m, 0:FIELDS, :] = atm_ref[m] - total
        anom_ref[m, FIELDS:16, :] = jnp.broadcast_to(
            state_ref[pl.ds(m, 1), :] - sst_mean, (16 - FIELDS, CELLS)
        )
        return carry

    lax.fori_loop(0, MEM, one, 0, unroll=4)


def side_kernel(meta_ref, state_ref, before_ref, after_ref, right_ref, left_ref):
    lane = lanes()
    state = state_ref[...]
    before = before_ref[...]
    after = after_ref[...]
    columns = jnp.where(lane % AY >= 8, before, after)
    turned = pltpu.roll(columns, 64, 1)
    right = jnp.where(lane >= 64, state, turned)
    left = jnp.where(lane < 64, state, turned)
    meta = meta_ref[...]

    def put(block, start, record, shift):
        moved = pltpu.roll(record, shift, 1) if shift else record
        return jnp.where((lane >= start) & (lane < start + 3), moved, block)

    for n, record in enumerate((meta, before, after)):
        right = put(right, META + 3 * n, record, 3 * n)
        left = put(left, 32 + META + 3 * n, record, 32 + 3 * n)
    right_ref[...] = right
    left_ref[...] = left


def views(blocks):
    lane = lanes()
    y = lane % AY
    x = lane // AY
    m0, m1, h0, h1 = blocks

    def up(a, b):
        return jnp.where(y == 15, pltpu.roll(b, 15, 1), pltpu.roll(a, 127, 1))

    def down(a, b):
        return jnp.where(y == 0, pltpu.roll(b, 113, 1), pltpu.roll(a, 1, 1))

    rows = {
        0: blocks,
        1: (up(m0, h0), up(m1, h1), up(h0, m0), up(h1, m1)),
        -1: (down(m0, h0), down(m1, h1), down(h0, m0), down(h1, m1)),
    }
    out = {}
    for dy, (a0, a1, b0, b1) in rows.items():
        out[0, dy] = (a0, a1, b0, b1)
        for dx, edge, shift in ((1, 0, 112), (-1, 7, 16)):

            def pair(u, v):
                return (
                    pltpu.roll(jnp.where(x == edge, v, u), shift, 1),
                    pltpu.roll(jnp.where(x == edge, u, v), shift, 1),
                )

            out[dx, dy] = pair(a0, a1) + pair(b0, b1)
    return out


def own_views(blocks):
    return {key: value[0] for key, value in views(blocks).items()}


def analysis_kernel(
    flag_ref, meta_ref, state_ref, before_ref, after_ref, west_ref, east_ref, mean_ref, anom_ref,
    post_mean_ref, post_anom_ref, first_ref, second_ref, work_ref,
):
    lane = lanes()
    y = lane % AY
    low_x = lane < 64
    high_y = y >= 8
    has_west = flag_ref[0]
    has_east = flag_ref[1]
    has_before = flag_ref[2]
    has_after = flag_ref[3]
    west = west_ref[...]
    east = east_ref[...]
    fields = [
        state_ref[...],
        jnp.where(low_x, east, west),
        jnp.where(high_y, before_ref[...], after_ref[...]),
        pltpu.roll(jnp.where(low_x, west, east), 64, 1),
    ]
    means = [jnp.sum(field, axis=0, keepdims=True) / MEM for field in fields]
    anoms = [field - mean for field, mean in zip(fields, means)]
    side_x = jnp.where(low_x, has_east, has_west)
    side_y = jnp.where(high_y, has_before, has_after)
    open_lane = [jnp.ones_like(side_x), side_x, side_y, side_x * side_y]

    def weights(batch, anoms, means):
        rows = pl.ds(batch * OB, OB)

        def column(ref, at):
            return jnp.broadcast_to(ref[rows, at : at + 1], (OB, CELLS))

        def record(block, n):
            if block == 0:
                return column(meta_ref, META + n)
            if block == 1:
                return jnp.where(
                    low_x, column(east_ref, 32 + META + n), column(west_ref, META + n)
                )
            if block == 2:
                return jnp.where(
                    high_y, column(before_ref, META + n), column(after_ref, META + n)
                )
            return jnp.where(
                low_x,
                jnp.where(
                    high_y,
                    column(east_ref, 32 + META + 3 + n),
                    column(east_ref, 32 + META + 6 + n),
                ),
                jnp.where(
                    high_y, column(west_ref, META + 3 + n), column(west_ref, META + 6 + n)
                ),
            )

        pulls, damped = [], []
        for block in range(4):
            anom, mean = anoms[block], means[block]
            variance = jnp.sum(anom * anom, axis=0, keepdims=True) / (MEM - 1)
            here = (record(block, 0) == lane.astype(f32)) & (open_lane[block] > 0)
            error = record(block, 2)
            denominator = variance + error
            pull = (record(block, 1) - mean) / denominator
            damp = 1.0 / (denominator + jnp.sqrt(error * denominator))
            pulls.append(jnp.sum(jnp.where(here, pull, 0.0), axis=0, keepdims=True))
            damped.append(jnp.sum(jnp.where(here, damp, 0.0), axis=0, keepdims=True))
        return pulls, damped

    def spread(rows):
        return [jnp.broadcast_to(row, (8, CELLS)) for row in rows]

    pulls, damped = weights(0, anoms, means)
    shifted = views(anoms)
    for n, key in enumerate(OFFSETS):
        first_ref[n] = shifted[key][0]
    pull_views = views(spread(pulls))
    damp_views = views(spread(damped))

    def scale(key):
        return TAPER[key[0] ** 2 + key[1] ** 2] / (MEM - 1)

    next_means, next_anoms = [], []
    for block in range(4):
        step = jnp.zeros_like(means[block])
        moved = anoms[block]
        for key in OFFSETS:
            view = shifted[key][block]
            covariance = jnp.sum(view * anoms[block], axis=0, keepdims=True) * scale(key)
            step = step + covariance * pull_views[key][block][0:1]
            moved = moved - (covariance * damp_views[key][block][0:1]) * view
        next_means.append(means[block] + step)
        next_anoms.append(moved)
    next_pulls, next_damped = weights(1, next_anoms, next_means)
    next_shifted = own_views(next_anoms)
    for n, key in enumerate(OFFSETS):
        second_ref[n] = next_shifted[key]
    next_pull_views = own_views(spread(next_pulls))
    next_damp_views = own_views(spread(next_damped))

    zero = jnp.zeros((16, CELLS), f32)

    def cov_first(m, sums):
        block = anom_ref[m]
        return tuple(s + block * first_ref[n, pl.ds(m, 1), :] for n, s in enumerate(sums))

    sums = lax.fori_loop(0, MEM, cov_first, (zero,) * 9, unroll=2)
    mean = mean_ref[...]
    gains = []
    for n, key in enumerate(OFFSETS):
        covariance = sums[n] * scale(key)
        mean = mean + covariance * pull_views[key][0][0:1]
        gains.append(covariance * damp_views[key][0][0:1])

    def step_first(m, sums):
        block = anom_ref[m]
        for n in range(9):
            block = block - gains[n] * first_ref[n, pl.ds(m, 1), :]
        work_ref[m] = block
        return tuple(s + block * second_ref[n, pl.ds(m, 1), :] for n, s in enumerate(sums))

    sums = lax.fori_loop(0, MEM, step_first, (zero,) * 9)
    last = []
    for n, key in enumerate(OFFSETS):
        covariance = sums[n] * scale(key)
        mean = mean + covariance * next_pull_views[key][0:1]
        last.append(covariance * next_damp_views[key][0:1])
    post_mean_ref[...] = mean[0:COMP]

    def step_second(m, carry):
        block = work_ref[m]
        for n in range(9):
            block = block - last[n] * second_ref[n, pl.ds(m, 1), :]
        post_anom_ref[m] = block[0:COMP]
        return carry

    lax.fori_loop(0, MEM, step_second, 0, unroll=2)


VMEM = pl.BlockSpec(memory_space=pltpu.VMEM)
SMEM = pl.BlockSpec(memory_space=pltpu.SMEM)


def flat(*shape):
    return jax.ShapeDtypeStruct(shape, f32)


def local(
    atm_members,
    ocean_members,
    remap_weights,
    pair_src,
    obs_cell,
    obs_value,
    obs_error,
    obs_live,
    obs_order,
):
    at_x = lax.axis_index("gx")
    at_y = lax.axis_index("gy")
    rows = lax.axis_size("gy")
    own = ocean_members[0, 0]
    before = ring(own, "gy", 1)
    after = ring(own, "gy", -1)
    tiles = [own, before, after]
    for first in (0, 1):
        tiles += [swap(tile, "gx", first) for tile in (own, before, after)]
    source = pair_src[0, 0]
    step_x = source // rows - at_x
    step_y = source % rows - at_y
    side = jnp.where(step_x == 0, 0, jnp.where((step_x == 1) == (at_x % 2 == 0), 1, 2))
    select = side * 3 + jnp.where(step_y == 0, 0, jnp.where(step_y < 0, 1, 2))

    order = obs_order[0, 0][:, None] == jnp.arange(OBS_DEV, dtype=jnp.int32)[None, :]

    def ordered(values):
        return jnp.sum(jnp.where(order, values[None, :], 0.0), axis=1, keepdims=True)

    cell = jnp.where(obs_live[0, 0] > 0, obs_cell[0, 0], -1).astype(f32)
    lane = jnp.arange(CELLS, dtype=jnp.int32)[None, :]
    meta = jnp.where(
        lane == META,
        ordered(cell),
        jnp.where(
            lane == META + 1,
            ordered(obs_value[0, 0]),
            jnp.where(lane == META + 2, ordered(obs_error[0, 0]), 0.0),
        ),
    )
    meta = jnp.pad(meta, ((0, MEM - OBS_DEV), (0, 0)))
    flags = jnp.stack(
        [at_x > 0, at_x < lax.axis_size("gx") - 1, at_y > 0, at_y < rows - 1]
    ).astype(jnp.int32)

    state, message = pl.pallas_call(
        remap_kernel,
        in_specs=[SMEM, VMEM, VMEM] + [VMEM] * 9,
        out_specs=[VMEM, VMEM],
        out_shape=[flat(MEM, CELLS), flat(MEM, CELLS)],
        name="remap",
    )(select, meta, remap_weights[0, 0], *tiles)
    from_before = ring(message, "gy", 1)
    from_after = ring(message, "gy", -1)
    mean, anomaly = pl.pallas_call(
        anomaly_kernel,
        in_specs=[VMEM, VMEM],
        out_specs=[VMEM, VMEM],
        out_shape=[flat(16, CELLS), flat(MEM, 16, CELLS)],
        name="anomaly",
    )(atm_members[0, 0], state)
    to_right, to_left = pl.pallas_call(
        side_kernel,
        in_specs=[VMEM] * 4,
        out_specs=[VMEM, VMEM],
        out_shape=[flat(MEM, CELLS), flat(MEM, CELLS)],
        name="side",
    )(meta, state, from_before, from_after)
    from_west = ring(to_right, "gx", 1)
    from_east = ring(to_left, "gx", -1)
    post_mean, post_anom = pl.pallas_call(
        analysis_kernel,
        in_specs=[SMEM] + [VMEM] * 8,
        out_specs=[VMEM, VMEM],
        out_shape=[flat(COMP, CELLS), flat(MEM, COMP, CELLS)],
        scratch_shapes=[
            pltpu.VMEM((9, MEM, CELLS), f32),
            pltpu.VMEM((9, MEM, CELLS), f32),
            pltpu.VMEM((MEM, 16, CELLS), f32),
        ],
        name="analysis",
    )(flags, meta, state, from_before, from_after, from_west, from_east, mean, anomaly)
    return post_mean[None, None], post_anom[None, None]


def solution(mesh):
    in_specs = (
        P("gx", "gy", None, None, None),
        P("gx", "gy", None, None),
        P("gx", "gy", None, None, None),
        P("gx", "gy", None),
        P("gx", "gy", None),
        P("gx", "gy", None),
        P("gx", "gy", None),
        P("gx", "gy", None),
        P("gx", "gy", None),
    )
    out_specs = (P("gx", "gy", None, None), P("gx", "gy", None, None, None))
    return jax.shard_map(local, mesh=mesh, in_specs=in_specs, out_specs=out_specs, check_vma=False)
```

```python
import functools

import jax
import jax.numpy as jnp
from jax import lax
from jax.experimental import pallas as pl
from jax.experimental.pallas import tpu as pltpu
from jax.sharding import PartitionSpec as P

MEM = 80
AX = 8
AY = 16
OCN_DEV = 1024
OB = 32
NB = 2
K = 4
FIELDS = 12
COMP = 13
CELLS = 128
OBS_DEV = 64

f32 = jnp.float32
META = 4
TAPER = {0: 1.0, 1: 0.5625, 2: 0.25}
OFFSETS = [(dx, dy) for dx in (-1, 0, 1) for dy in (-1, 0, 1)]


def ring(block, axis, step):
    count = lax.axis_size(axis)
    return lax.ppermute(block, axis, [(i, (i + step) % count) for i in range(count)])


def swap(block, axis, first):
    count = lax.axis_size(axis)
    pairs = []
    for at in range(first, count + first, 2):
        low, high = at % count, (at + 1) % count
        pairs += [(low, high), (high, low)]
    return lax.ppermute(block, axis, sorted(pairs))


def lanes(rows=1):
    return lax.broadcasted_iota(jnp.int32, (rows, CELLS), 1)


def prepare_kernel(
    atm_hbm, weight_hbm, order_ref, cell_ref, live_ref, value_ref, error_ref,
    weight_ref, anom_ref, mean_ref, meta_ref, sem_ref,
):
    weights = pltpu.make_async_copy(weight_hbm, weight_ref, sem_ref.at[0])
    fields = pltpu.make_async_copy(atm_hbm, anom_ref, sem_ref.at[1])
    fields.start()
    weights.start()
    order = jnp.transpose(jnp.broadcast_to(order_ref[...], (OBS_DEV, OBS_DEV)))
    taken = order == lax.broadcasted_iota(jnp.int32, (OBS_DEV, OBS_DEV), 1)
    lane = lanes(OBS_DEV)

    def ordered(row):
        picked = jnp.sum(jnp.where(taken, row, 0.0), axis=1, keepdims=True)
        return jnp.broadcast_to(picked, (OBS_DEV, CELLS))

    cell = jnp.where(live_ref[...] > 0, cell_ref[...], -1).astype(f32)
    meta_ref[...] = jnp.zeros_like(meta_ref)
    meta_ref[0:OBS_DEV, :] = jnp.where(
        lane == META,
        ordered(cell),
        jnp.where(lane == META + 1, ordered(value_ref[...]), ordered(error_ref[...])),
    )
    fields.wait()
    mean_ref[...] = jnp.zeros_like(mean_ref)
    for v in range(FIELDS):
        field = anom_ref[v]
        mean = jnp.sum(field, axis=0, keepdims=True) / MEM
        mean_ref[v : v + 1, :] = mean
        anom_ref[v] = field - mean
    weights.wait()


def remap_kernel(sel_ref, meta_ref, w_ref, *refs):
    tiles, (state_ref, message_ref) = refs[:9], refs[9:]
    state_ref[...] = jnp.zeros_like(state_ref)

    def one(k, carry):
        for index, tile in enumerate(tiles):

            @pl.when(sel_ref[k] == index)
            def _():
                state_ref[...] += jnp.dot(tile[...], w_ref[k], preferred_element_type=f32)

        return carry

    lax.fori_loop(0, K, one, 0)
    lane = lanes()
    message_ref[...] = jnp.where(
        (lane >= META) & (lane < META + 3), meta_ref[...], state_ref[...]
    )


def side_kernel(meta_ref, state_ref, before_ref, after_ref, right_ref, left_ref):
    lane = lanes()
    state = state_ref[...]
    before = before_ref[...]
    after = after_ref[...]
    columns = jnp.where(lane % AY >= 8, before, after)
    turned = pltpu.roll(columns, 64, 1)
    right = jnp.where(lane >= 64, state, turned)
    left = jnp.where(lane < 64, state, turned)
    meta = meta_ref[...]

    def put(block, start, record, shift):
        moved = pltpu.roll(record, shift, 1) if shift else record
        return jnp.where((lane >= start) & (lane < start + 3), moved, block)

    for n, record in enumerate((meta, before, after)):
        right = put(right, META + 3 * n, record, 3 * n)
        left = put(left, 32 + META + 3 * n, record, 32 + 3 * n)
    right_ref[...] = right
    left_ref[...] = left


def views(blocks):
    lane = lanes()
    y = lane % AY
    x = lane // AY
    m0, m1, h0, h1 = blocks

    def up(a, b):
        return jnp.where(y == 15, pltpu.roll(b, 15, 1), pltpu.roll(a, 127, 1))

    def down(a, b):
        return jnp.where(y == 0, pltpu.roll(b, 113, 1), pltpu.roll(a, 1, 1))

    rows = {
        0: blocks,
        1: (up(m0, h0), up(m1, h1), up(h0, m0), up(h1, m1)),
        -1: (down(m0, h0), down(m1, h1), down(h0, m0), down(h1, m1)),
    }
    out = {}
    for dy, (a0, a1, b0, b1) in rows.items():
        out[0, dy] = (a0, a1, b0, b1)
        for dx, edge, shift in ((1, 0, 112), (-1, 7, 16)):

            def pair(u, v):
                return (
                    pltpu.roll(jnp.where(x == edge, v, u), shift, 1),
                    pltpu.roll(jnp.where(x == edge, u, v), shift, 1),
                )

            out[dx, dy] = pair(a0, a1) + pair(b0, b1)
    return out


def own_views(blocks):
    lane = lanes()
    y = lane % AY
    x = lane // AY
    m0, m1, h0, h1 = blocks
    rows = {0: (m0, m1), 1: [], -1: []}
    for a, b in ((m0, h0), (m1, h1)):
        rows[1].append(jnp.where(y == 15, pltpu.roll(b, 15, 1), pltpu.roll(a, 127, 1)))
        rows[-1].append(jnp.where(y == 0, pltpu.roll(b, 113, 1), pltpu.roll(a, 1, 1)))
    out = {}
    for dy, (u, v) in rows.items():
        out[0, dy] = u
        out[1, dy] = pltpu.roll(jnp.where(x == 0, v, u), 112, 1)
        out[-1, dy] = pltpu.roll(jnp.where(x == 7, v, u), 16, 1)
    return out


ROWS = MEM // 8


def group(r):
    return pl.ds(pl.multiple_of(r * 8, 8), 8)


def total(block):
    return jnp.sum(block, axis=0, keepdims=True)


def analysis_kernel(
    meta_ref, state_ref, before_ref, after_ref, west_ref, east_ref, mean_ref, anom_ref,
    post_mean_hbm, post_anom_hbm,
    field_ref, moved_ref, first_ref, second_ref, out_ref, out_mean_ref, sem_ref,
):
    lane = lanes()
    y = lane % AY
    low_x = lane < 64
    high_y = y >= 8
    at_x, at_y = lax.axis_index("gx"), lax.axis_index("gy")
    has_west = (at_x > 0).astype(jnp.int32)
    has_east = (at_x < lax.axis_size("gx") - 1).astype(jnp.int32)
    has_before = (at_y > 0).astype(jnp.int32)
    has_after = (at_y < lax.axis_size("gy") - 1).astype(jnp.int32)
    west = west_ref[...]
    east = east_ref[...]
    fields = [
        state_ref[...],
        jnp.where(low_x, east, west),
        jnp.where(high_y, before_ref[...], after_ref[...]),
        pltpu.roll(jnp.where(low_x, west, east), 64, 1),
    ]
    means = [total(field) / MEM for field in fields]
    squares = []
    for block in range(4):
        anom = fields[block] - means[block]
        field_ref[block] = anom
        squares.append(total(anom * anom))
    side_x = jnp.where(low_x, has_east, has_west)
    side_y = jnp.where(high_y, has_before, has_after)
    open_lane = [jnp.ones_like(side_x), side_x, side_y, side_x * side_y]

    def weights(batch, squares, means):
        rows = pl.ds(batch * OB, OB)

        def column(ref, at):
            return jnp.broadcast_to(ref[rows, at : at + 1], (OB, CELLS))

        def record(block, n):
            if block == 0:
                return column(meta_ref, META + n)
            if block == 1:
                return jnp.where(
                    low_x, column(east_ref, 32 + META + n), column(west_ref, META + n)
                )
            if block == 2:
                return jnp.where(
                    high_y, column(before_ref, META + n), column(after_ref, META + n)
                )
            return jnp.where(
                low_x,
                jnp.where(
                    high_y,
                    column(east_ref, 32 + META + 3 + n),
                    column(east_ref, 32 + META + 6 + n),
                ),
                jnp.where(
                    high_y, column(west_ref, META + 3 + n), column(west_ref, META + 6 + n)
                ),
            )

        pulls, damped = [], []
        for block in range(4):
            variance = squares[block] / (MEM - 1)
            here = (record(block, 0) == lane.astype(f32)) & (open_lane[block] > 0)
            error = record(block, 2)
            denominator = variance + error
            pull = (record(block, 1) - means[block]) / denominator
            damp = 1.0 / (denominator + jnp.sqrt(error * denominator))
            pulls.append(total(jnp.where(here, pull, 0.0)))
            damped.append(total(jnp.where(here, damp, 0.0)))
        return pulls, damped

    def spread(rows):
        return [jnp.broadcast_to(row, (8, CELLS)) for row in rows]

    def scale(key):
        return TAPER[key[0] ** 2 + key[1] ** 2] / (MEM - 1)

    zero = jnp.zeros((8, CELLS), f32)

    pulls, damped = weights(0, squares, means)
    pull_views = views(spread(pulls))
    damp_views = views(spread(damped))

    def shift_first(r, sums):
        at = group(r)
        blocks = [field_ref[block, at, :] for block in range(4)]
        shifted = views(blocks)
        out = []
        for n, key in enumerate(OFFSETS):
            for block in range(4):
                first_ref[block, n, at, :] = shifted[key][block]
                out.append(sums[n * 4 + block] + shifted[key][block] * blocks[block])
        return tuple(out)

    sums = lax.fori_loop(0, ROWS, shift_first, (zero,) * 36)
    next_means, next_squares = [], []
    for block in range(4):
        step = jnp.zeros_like(means[block])
        gains = []
        for n, key in enumerate(OFFSETS):
            covariance = total(sums[n * 4 + block]) * scale(key)
            step = step + covariance * pull_views[key][block][0:1]
            gains.append(covariance * damp_views[key][block][0:1])
        square = zero
        for r in range(ROWS):
            at = slice(8 * r, 8 * r + 8)
            moved = field_ref[block, at, :]
            for n in range(9):
                moved = moved - gains[n] * first_ref[block, n, at, :]
            moved_ref[block, at, :] = moved
            square = square + moved * moved
        next_means.append(means[block] + step)
        next_squares.append(total(square))
    next_pulls, next_damped = weights(1, next_squares, next_means)
    next_pull_views = own_views(spread(next_pulls))
    next_damp_views = own_views(spread(next_damped))

    def shift_second(r, sums):
        at = group(r)
        blocks = [moved_ref[block, at, :] for block in range(4)]
        shifted = own_views(blocks)
        out = []
        for n, key in enumerate(OFFSETS):
            second_ref[n, at, :] = shifted[key]
            out.append(sums[n] + shifted[key] * blocks[0])
        return tuple(out)

    sums = lax.fori_loop(0, ROWS, shift_second, (zero,) * 9)

    def finish(sums, mean):
        gains = []
        for n, key in enumerate(OFFSETS):
            covariance = total(sums[n]) * scale(key)
            mean = mean + covariance * next_pull_views[key][0:1]
            gains.append(covariance * next_damp_views[key][0:1])
        return gains, mean

    gains, mean = finish(sums, next_means[0])
    out_mean_ref[FIELDS] = mean
    for r in range(ROWS):
        at = slice(8 * r, 8 * r + 8)
        block = moved_ref[0, at, :]
        for n in range(9):
            block = block - gains[n] * second_ref[n, at, :]
        out_ref[FIELDS, at, :] = block

    def send(v, count):
        return pltpu.make_async_copy(
            out_ref.at[pl.ds(v, count)], post_anom_hbm.at[pl.ds(v, count)], sem_ref.at[0]
        )

    def pair(g, carry):
        comps = [2 * g, 2 * g + 1]
        sums = [[zero] * 9, [zero] * 9]
        for r in range(ROWS):
            at = slice(8 * r, 8 * r + 8)
            shifted = [first_ref[0, n, at, :] for n in range(9)]
            for i, v in enumerate(comps):
                block = anom_ref[v, at, :]
                sums[i] = [s + block * w for s, w in zip(sums[i], shifted)]
        means, gains = [], []
        for i, v in enumerate(comps):
            mean = mean_ref[pl.ds(v, 1), :]
            own = []
            for n, key in enumerate(OFFSETS):
                covariance = total(sums[i][n]) * scale(key)
                mean = mean + covariance * pull_views[key][0][0:1]
                own.append(covariance * damp_views[key][0][0:1])
            means.append(mean)
            gains.append(own)
        sums = [[zero] * 9, [zero] * 9]
        for r in range(ROWS):
            at = slice(8 * r, 8 * r + 8)
            shifted = [first_ref[0, n, at, :] for n in range(9)]
            later = [second_ref[n, at, :] for n in range(9)]
            for i, v in enumerate(comps):
                block = anom_ref[v, at, :]
                for n in range(9):
                    block = block - gains[i][n] * shifted[n]
                out_ref[v, at, :] = block
                sums[i] = [s + block * w for s, w in zip(sums[i], later)]
        for i, v in enumerate(comps):
            gains[i], mean = finish(sums[i], means[i])
            out_mean_ref[v] = mean
        for r in range(ROWS):
            at = slice(8 * r, 8 * r + 8)
            later = [second_ref[n, at, :] for n in range(9)]
            for i, v in enumerate(comps):
                block = out_ref[v, at, :]
                for n in range(9):
                    block = block - gains[i][n] * later[n]
                out_ref[v, at, :] = block
        send(2 * g, 2).start()
        return carry

    send(FIELDS, 1).start()
    lax.fori_loop(0, FIELDS // 2, pair, 0)
    last = pltpu.make_async_copy(out_mean_ref, post_mean_hbm, sem_ref.at[1])
    last.start()
    pltpu.make_async_copy(out_ref, post_anom_hbm, sem_ref.at[0]).wait()
    last.wait()


VMEM = pl.BlockSpec(memory_space=pltpu.VMEM)
SMEM = pl.BlockSpec(memory_space=pltpu.SMEM)
ANY = pl.BlockSpec(memory_space=pl.ANY)
LIMIT = pltpu.CompilerParams(vmem_limit_bytes=8 << 20)


def flat(*shape):
    return jax.ShapeDtypeStruct(shape, f32)


def local(
    atm_members,
    ocean_members,
    remap_weights,
    pair_src,
    obs_cell,
    obs_value,
    obs_error,
    obs_live,
    obs_order,
):
    at_x = lax.axis_index("gx")
    at_y = lax.axis_index("gy")
    rows = lax.axis_size("gy")
    own = ocean_members[0, 0]
    before = ring(own, "gy", 1)
    after = ring(own, "gy", -1)
    tiles = [own, before, after]
    for first in (0, 1):
        tiles += [swap(tile, "gx", first) for tile in (own, before, after)]
    source = pair_src[0, 0]
    step_x = source // rows - at_x
    step_y = source % rows - at_y
    side = jnp.where(step_x == 0, 0, jnp.where((step_x == 1) == (at_x % 2 == 0), 1, 2))
    select = side * 3 + jnp.where(step_y == 0, 0, jnp.where(step_y < 0, 1, 2))

    weights, anomaly, mean, meta = pl.pallas_call(
        prepare_kernel,
        in_specs=[ANY, ANY] + [VMEM] * 5,
        out_specs=[VMEM] * 4,
        out_shape=[
            jax.ShapeDtypeStruct((K, OCN_DEV, CELLS), jnp.bfloat16),
            flat(FIELDS, MEM, CELLS),
            flat(16, CELLS),
            flat(MEM, CELLS),
        ],
        scratch_shapes=[pltpu.SemaphoreType.DMA((2,))],
        name="prepare",
        compiler_params=LIMIT,
    )(
        jnp.transpose(atm_members[0, 0], (1, 0, 2)),
        remap_weights[0, 0],
        obs_order[0],
        obs_cell[0],
        obs_live[0],
        obs_value[0],
        obs_error[0],
    )
    state, message = pl.pallas_call(
        remap_kernel,
        in_specs=[SMEM, VMEM, VMEM] + [VMEM] * 9,
        out_specs=[VMEM, VMEM],
        out_shape=[flat(MEM, CELLS), flat(MEM, CELLS)],
        name="remap",
        compiler_params=LIMIT,
    )(select, meta, weights, *tiles)
    from_before = ring(message, "gy", 1)
    from_after = ring(message, "gy", -1)
    to_right, to_left = pl.pallas_call(
        side_kernel,
        in_specs=[VMEM] * 4,
        out_specs=[VMEM, VMEM],
        out_shape=[flat(MEM, CELLS), flat(MEM, CELLS)],
        name="side",
        compiler_params=LIMIT,
    )(meta, state, from_before, from_after)
    from_west = ring(to_right, "gx", 1)
    from_east = ring(to_left, "gx", -1)
    post_mean, post_anom = pl.pallas_call(
        analysis_kernel,
        in_specs=[VMEM] * 8,
        out_specs=[ANY, ANY],
        out_shape=[flat(COMP, 1, CELLS), flat(COMP, MEM, CELLS)],
        scratch_shapes=[
            pltpu.VMEM((4, MEM, CELLS), f32),
            pltpu.VMEM((4, MEM, CELLS), f32),
            pltpu.VMEM((4, 9, MEM, CELLS), f32),
            pltpu.VMEM((9, MEM, CELLS), f32),
            pltpu.VMEM((COMP, MEM, CELLS), f32),
            pltpu.VMEM((COMP, 1, CELLS), f32),
            pltpu.SemaphoreType.DMA((2,)),
        ],
        name="analysis",
        compiler_params=LIMIT,
    )(meta, state, from_before, from_after, from_west, from_east, mean, anomaly)
    post_mean = jnp.transpose(post_mean, (1, 0, 2))
    post_anom = jnp.transpose(post_anom, (1, 0, 2))
    return post_mean[None], post_anom[None, None]


def solution(mesh):
    in_specs = (
        P("gx", "gy", None, None, None),
        P("gx", "gy", None, None),
        P("gx", "gy", None, None, None),
        P("gx", "gy", None),
        P("gx", "gy", None),
        P("gx", "gy", None),
        P("gx", "gy", None),
        P("gx", "gy", None),
        P("gx", "gy", None),
    )
    out_specs = (P("gx", "gy", None, None), P("gx", "gy", None, None, None))
    return jax.shard_map(local, mesh=mesh, in_specs=in_specs, out_specs=out_specs, check_vma=False)
```

```python
import functools

import jax
import jax.numpy as jnp
from jax import lax
from jax.experimental import pallas as pl
from jax.experimental.pallas import tpu as pltpu
from jax.sharding import PartitionSpec as P

MEM = 80
AX = 8
AY = 16
OCN_DEV = 1024
OB = 32
NB = 2
K = 4
FIELDS = 12
COMP = 13
CELLS = 128
OBS_DEV = 64

f32 = jnp.float32
META = 4
TAPER = {0: 1.0, 1: 0.5625, 2: 0.25}
OFFSETS = [(dx, dy) for dx in (-1, 0, 1) for dy in (-1, 0, 1)]


def exchange(block, axis, first):
    count_x, count_y = lax.axis_size("gx"), lax.axis_size("gy")
    pairs = []
    for x in range(count_x):
        for y in range(count_y):
            at, count = (x, count_x) if axis == "gx" else (y, count_y)
            other = at ^ 1 if first == 0 else at - 1 + 2 * (at % 2)
            if not 0 <= other < count:
                to = (x, y ^ 1) if axis == "gx" else (x ^ 1, y)
            else:
                to = (other, y) if axis == "gx" else (x, other)
            pairs.append((x * count_y + y, to[0] * count_y + to[1]))
    return lax.ppermute(block, ("gx", "gy"), pairs)


def lanes(rows=1):
    return lax.broadcasted_iota(jnp.int32, (rows, CELLS), 1)


def prepare_kernel(
    atm_hbm, weight_hbm, order_ref, cell_ref, live_ref, value_ref, error_ref,
    weight_ref, anom_ref, mean_ref, meta_ref, sem_ref,
):
    weights = pltpu.make_async_copy(weight_hbm, weight_ref, sem_ref.at[0])
    fields = pltpu.make_async_copy(atm_hbm, anom_ref, sem_ref.at[1])
    fields.start()
    weights.start()
    order = jnp.transpose(jnp.broadcast_to(order_ref[...], (OBS_DEV, OBS_DEV)))
    taken = order == lax.broadcasted_iota(jnp.int32, (OBS_DEV, OBS_DEV), 1)
    lane = lanes(OBS_DEV)

    def ordered(row):
        picked = jnp.sum(jnp.where(taken, row, 0.0), axis=1, keepdims=True)
        return jnp.broadcast_to(picked, (OBS_DEV, CELLS))

    cell = jnp.where(live_ref[...] > 0, cell_ref[...], -1).astype(f32)
    meta_ref[...] = jnp.zeros_like(meta_ref)
    meta_ref[0:OBS_DEV, :] = jnp.where(
        lane == META,
        ordered(cell),
        jnp.where(lane == META + 1, ordered(value_ref[...]), ordered(error_ref[...])),
    )
    fields.wait()
    mean_ref[...] = jnp.zeros_like(mean_ref)
    for v in range(FIELDS):
        field = anom_ref[v]
        mean = jnp.sum(field, axis=0, keepdims=True) / MEM
        mean_ref[v : v + 1, :] = mean
        anom_ref[v] = field - mean
    weights.wait()


def remap_kernel(sel_ref, meta_ref, w_ref, *refs):
    tiles, (state_ref, message_ref) = refs[:9], refs[9:]
    state_ref[...] = jnp.zeros_like(state_ref)

    def one(k, carry):
        for index, tile in enumerate(tiles):

            @pl.when(sel_ref[k] == index)
            def _():
                state_ref[...] += jnp.dot(tile[...], w_ref[k], preferred_element_type=f32)

        return carry

    lax.fori_loop(0, K, one, 0)
    lane = lanes()
    message_ref[...] = jnp.where(
        (lane >= META) & (lane < META + 3), meta_ref[...], state_ref[...]
    )


def even(axis):
    return lax.axis_index(axis) % 2 == 0


def sides(low_ref, high_ref, axis):
    low, high = low_ref[...], high_ref[...]
    return jnp.where(even(axis), high, low), jnp.where(even(axis), low, high)


def side_kernel(meta_ref, state_ref, close_ref, far_ref, near_out_ref, far_out_ref):
    lane = lanes()
    state = state_ref[...]
    before, after = sides(close_ref, far_ref, "gy")
    columns = jnp.where(lane % AY >= 8, before, after)
    turned = pltpu.roll(columns, 64, 1)
    right = jnp.where(lane >= 64, state, turned)
    left = jnp.where(lane < 64, state, turned)
    meta = meta_ref[...]

    def put(block, start, record, shift):
        moved = pltpu.roll(record, shift, 1) if shift else record
        return jnp.where((lane >= start) & (lane < start + 3), moved, block)

    for n, record in enumerate((meta, before, after)):
        right = put(right, META + 3 * n, record, 3 * n)
        left = put(left, 32 + META + 3 * n, record, 32 + 3 * n)
    near_out_ref[...] = jnp.where(even("gx"), right, left)
    far_out_ref[...] = jnp.where(even("gx"), left, right)


def views(blocks):
    lane = lanes()
    y = lane % AY
    x = lane // AY
    m0, m1, h0, h1 = blocks

    def up(a, b):
        return jnp.where(y == 15, pltpu.roll(b, 15, 1), pltpu.roll(a, 127, 1))

    def down(a, b):
        return jnp.where(y == 0, pltpu.roll(b, 113, 1), pltpu.roll(a, 1, 1))

    rows = {
        0: blocks,
        1: (up(m0, h0), up(m1, h1), up(h0, m0), up(h1, m1)),
        -1: (down(m0, h0), down(m1, h1), down(h0, m0), down(h1, m1)),
    }
    out = {}
    for dy, (a0, a1, b0, b1) in rows.items():
        out[0, dy] = (a0, a1, b0, b1)
        for dx, edge, shift in ((1, 0, 112), (-1, 7, 16)):

            def pair(u, v):
                return (
                    pltpu.roll(jnp.where(x == edge, v, u), shift, 1),
                    pltpu.roll(jnp.where(x == edge, u, v), shift, 1),
                )

            out[dx, dy] = pair(a0, a1) + pair(b0, b1)
    return out


def own_views(blocks):
    lane = lanes()
    y = lane % AY
    x = lane // AY
    m0, m1, h0, h1 = blocks
    rows = {0: (m0, m1), 1: [], -1: []}
    for a, b in ((m0, h0), (m1, h1)):
        rows[1].append(jnp.where(y == 15, pltpu.roll(b, 15, 1), pltpu.roll(a, 127, 1)))
        rows[-1].append(jnp.where(y == 0, pltpu.roll(b, 113, 1), pltpu.roll(a, 1, 1)))
    out = {}
    for dy, (u, v) in rows.items():
        out[0, dy] = u
        out[1, dy] = pltpu.roll(jnp.where(x == 0, v, u), 112, 1)
        out[-1, dy] = pltpu.roll(jnp.where(x == 7, v, u), 16, 1)
    return out


ROWS = MEM // 8


def group(r):
    return pl.ds(pl.multiple_of(r * 8, 8), 8)


def total(block):
    return jnp.sum(block, axis=0, keepdims=True)


def analysis_kernel(
    meta_ref, state_ref, near_y_ref, far_y_ref, near_x_ref, far_x_ref, mean_ref, anom_ref,
    post_mean_hbm, post_anom_hbm,
    field_ref, moved_ref, first_ref, second_ref, out_ref, out_mean_ref, sem_ref,
):
    lane = lanes()
    y = lane % AY
    low_x = lane < 64
    high_y = y >= 8
    at_x, at_y = lax.axis_index("gx"), lax.axis_index("gy")
    has_west = (at_x > 0).astype(jnp.int32)
    has_east = (at_x < lax.axis_size("gx") - 1).astype(jnp.int32)
    has_before = (at_y > 0).astype(jnp.int32)
    has_after = (at_y < lax.axis_size("gy") - 1).astype(jnp.int32)
    meta = meta_ref[...]
    before, after = sides(near_y_ref, far_y_ref, "gy")
    west, east = sides(near_x_ref, far_x_ref, "gx")
    fields = [
        state_ref[...],
        jnp.where(low_x, east, west),
        jnp.where(high_y, before, after),
        pltpu.roll(jnp.where(low_x, west, east), 64, 1),
    ]
    means = [total(field) / MEM for field in fields]
    squares = []
    for block in range(4):
        anom = fields[block] - means[block]
        field_ref[block] = anom
        squares.append(total(anom * anom))
    side_x = jnp.where(low_x, has_east, has_west)
    side_y = jnp.where(high_y, has_before, has_after)
    open_lane = [jnp.ones_like(side_x), side_x, side_y, side_x * side_y]

    def weights(batch, squares, means):
        rows = slice(batch * OB, batch * OB + OB)

        def column(block, at):
            return jnp.broadcast_to(block[rows, at : at + 1], (OB, CELLS))

        def record(block, n):
            if block == 0:
                return column(meta, META + n)
            if block == 1:
                return jnp.where(
                    low_x, column(east, 32 + META + n), column(west, META + n)
                )
            if block == 2:
                return jnp.where(
                    high_y, column(before, META + n), column(after, META + n)
                )
            return jnp.where(
                low_x,
                jnp.where(
                    high_y,
                    column(east, 32 + META + 3 + n),
                    column(east, 32 + META + 6 + n),
                ),
                jnp.where(
                    high_y, column(west, META + 3 + n), column(west, META + 6 + n)
                ),
            )

        pulls, damped = [], []
        for block in range(4):
            variance = squares[block] / (MEM - 1)
            here = (record(block, 0) == lane.astype(f32)) & (open_lane[block] > 0)
            error = record(block, 2)
            denominator = variance + error
            pull = (record(block, 1) - means[block]) / denominator
            damp = 1.0 / (denominator + jnp.sqrt(error * denominator))
            pulls.append(total(jnp.where(here, pull, 0.0)))
            damped.append(total(jnp.where(here, damp, 0.0)))
        return pulls, damped

    def spread(rows):
        return [jnp.broadcast_to(row, (8, CELLS)) for row in rows]

    def scale(key):
        return TAPER[key[0] ** 2 + key[1] ** 2] / (MEM - 1)

    zero = jnp.zeros((8, CELLS), f32)

    pulls, damped = weights(0, squares, means)
    pull_views = views(spread(pulls))
    damp_views = views(spread(damped))

    def shift_first(r, sums):
        at = group(r)
        blocks = [field_ref[block, at, :] for block in range(4)]
        shifted = views(blocks)
        out = []
        for n, key in enumerate(OFFSETS):
            for block in range(4):
                first_ref[block, n, at, :] = shifted[key][block]
                out.append(sums[n * 4 + block] + shifted[key][block] * blocks[block])
        return tuple(out)

    sums = lax.fori_loop(0, ROWS, shift_first, (zero,) * 36)
    next_means, next_squares = [], []
    for block in range(4):
        step = jnp.zeros_like(means[block])
        gains = []
        for n, key in enumerate(OFFSETS):
            covariance = total(sums[n * 4 + block]) * scale(key)
            step = step + covariance * pull_views[key][block][0:1]
            gains.append(covariance * damp_views[key][block][0:1])
        square = zero
        for r in range(ROWS):
            at = slice(8 * r, 8 * r + 8)
            moved = field_ref[block, at, :]
            for n in range(9):
                moved = moved - gains[n] * first_ref[block, n, at, :]
            moved_ref[block, at, :] = moved
            square = square + moved * moved
        next_means.append(means[block] + step)
        next_squares.append(total(square))
    next_pulls, next_damped = weights(1, next_squares, next_means)
    next_pull_views = own_views(spread(next_pulls))
    next_damp_views = own_views(spread(next_damped))

    def shift_second(r, sums):
        at = group(r)
        blocks = [moved_ref[block, at, :] for block in range(4)]
        shifted = own_views(blocks)
        out = []
        for n, key in enumerate(OFFSETS):
            second_ref[n, at, :] = shifted[key]
            out.append(sums[n] + shifted[key] * blocks[0])
        return tuple(out)

    sums = lax.fori_loop(0, ROWS, shift_second, (zero,) * 9)

    def finish(sums, mean):
        gains = []
        for n, key in enumerate(OFFSETS):
            covariance = total(sums[n]) * scale(key)
            mean = mean + covariance * next_pull_views[key][0:1]
            gains.append(covariance * next_damp_views[key][0:1])
        return gains, mean

    gains, mean = finish(sums, next_means[0])
    out_mean_ref[FIELDS] = mean
    for r in range(ROWS):
        at = slice(8 * r, 8 * r + 8)
        block = moved_ref[0, at, :]
        for n in range(9):
            block = block - gains[n] * second_ref[n, at, :]
        out_ref[FIELDS, at, :] = block

    def send(v, count):
        return pltpu.make_async_copy(
            out_ref.at[pl.ds(v, count)], post_anom_hbm.at[pl.ds(v, count)], sem_ref.at[0]
        )

    def pair(g, carry):
        comps = [2 * g, 2 * g + 1]
        sums = [[zero] * 9, [zero] * 9]
        for r in range(ROWS):
            at = slice(8 * r, 8 * r + 8)
            shifted = [first_ref[0, n, at, :] for n in range(9)]
            for i, v in enumerate(comps):
                block = anom_ref[v, at, :]
                sums[i] = [s + block * w for s, w in zip(sums[i], shifted)]
        means, gains = [], []
        for i, v in enumerate(comps):
            mean = mean_ref[pl.ds(v, 1), :]
            own = []
            for n, key in enumerate(OFFSETS):
                covariance = total(sums[i][n]) * scale(key)
                mean = mean + covariance * pull_views[key][0][0:1]
                own.append(covariance * damp_views[key][0][0:1])
            means.append(mean)
            gains.append(own)
        sums = [[zero] * 9, [zero] * 9]
        for r in range(ROWS):
            at = slice(8 * r, 8 * r + 8)
            shifted = [first_ref[0, n, at, :] for n in range(9)]
            later = [second_ref[n, at, :] for n in range(9)]
            for i, v in enumerate(comps):
                block = anom_ref[v, at, :]
                for n in range(9):
                    block = block - gains[i][n] * shifted[n]
                out_ref[v, at, :] = block
                sums[i] = [s + block * w for s, w in zip(sums[i], later)]
        for i, v in enumerate(comps):
            gains[i], mean = finish(sums[i], means[i])
            out_mean_ref[v] = mean
        for r in range(ROWS):
            at = slice(8 * r, 8 * r + 8)
            later = [second_ref[n, at, :] for n in range(9)]
            for i, v in enumerate(comps):
                block = out_ref[v, at, :]
                for n in range(9):
                    block = block - gains[i][n] * later[n]
                out_ref[v, at, :] = block
        send(2 * g, 2).start()
        return carry

    send(FIELDS, 1).start()
    lax.fori_loop(0, FIELDS // 2, pair, 0)
    last = pltpu.make_async_copy(out_mean_ref, post_mean_hbm, sem_ref.at[1])
    last.start()
    pltpu.make_async_copy(out_ref, post_anom_hbm, sem_ref.at[0]).wait()
    last.wait()


VMEM = pl.BlockSpec(memory_space=pltpu.VMEM)
SMEM = pl.BlockSpec(memory_space=pltpu.SMEM)
ANY = pl.BlockSpec(memory_space=pl.ANY)
LIMIT = pltpu.CompilerParams(vmem_limit_bytes=8 << 20)


def flat(*shape):
    return jax.ShapeDtypeStruct(shape, f32)


def local(
    atm_members,
    ocean_members,
    remap_weights,
    pair_src,
    obs_cell,
    obs_value,
    obs_error,
    obs_live,
    obs_order,
):
    at_x = lax.axis_index("gx")
    at_y = lax.axis_index("gy")
    rows = lax.axis_size("gy")
    own = ocean_members[0, 0]
    column = [own] + [exchange(own, "gy", first) for first in (0, 1)]
    tiles = list(column)
    for first in (0, 1):
        tiles += [exchange(tile, "gx", first) for tile in column]
    source = pair_src[0, 0]

    def slot(step, at):
        return jnp.where(step == 0, 0, jnp.where((step == 1) == (at % 2 == 0), 1, 2))

    select = slot(source // rows - at_x, at_x) * 3 + slot(source % rows - at_y, at_y)
    weights, anomaly, mean, meta = pl.pallas_call(
        prepare_kernel,
        in_specs=[ANY, ANY] + [VMEM] * 5,
        out_specs=[VMEM] * 4,
        out_shape=[
            jax.ShapeDtypeStruct((K, OCN_DEV, CELLS), jnp.bfloat16),
            flat(FIELDS, MEM, CELLS),
            flat(16, CELLS),
            flat(MEM, CELLS),
        ],
        scratch_shapes=[pltpu.SemaphoreType.DMA((2,))],
        name="prepare",
        compiler_params=LIMIT,
    )(
        jnp.transpose(atm_members[0, 0], (1, 0, 2)),
        remap_weights[0, 0],
        obs_order[0],
        obs_cell[0],
        obs_live[0],
        obs_value[0],
        obs_error[0],
    )
    state, message = pl.pallas_call(
        remap_kernel,
        in_specs=[SMEM, VMEM, VMEM] + [VMEM] * 9,
        out_specs=[VMEM, VMEM],
        out_shape=[flat(MEM, CELLS), flat(MEM, CELLS)],
        name="remap",
        compiler_params=LIMIT,
    )(select, meta, weights, *tiles)
    near_y = exchange(message, "gy", 0)
    far_y = exchange(message, "gy", 1)
    near_out, far_out = pl.pallas_call(
        side_kernel,
        in_specs=[VMEM] * 4,
        out_specs=[VMEM, VMEM],
        out_shape=[flat(MEM, CELLS), flat(MEM, CELLS)],
        name="side",
        compiler_params=LIMIT,
    )(meta, state, near_y, far_y)
    near_x = exchange(near_out, "gx", 0)
    far_x = exchange(far_out, "gx", 1)
    post_mean, post_anom = pl.pallas_call(
        analysis_kernel,
        in_specs=[VMEM] * 8,
        out_specs=[ANY, ANY],
        out_shape=[flat(COMP, 1, CELLS), flat(COMP, MEM, CELLS)],
        scratch_shapes=[
            pltpu.VMEM((4, MEM, CELLS), f32),
            pltpu.VMEM((4, MEM, CELLS), f32),
            pltpu.VMEM((4, 9, MEM, CELLS), f32),
            pltpu.VMEM((9, MEM, CELLS), f32),
            pltpu.VMEM((COMP, MEM, CELLS), f32),
            pltpu.VMEM((COMP, 1, CELLS), f32),
            pltpu.SemaphoreType.DMA((2,)),
        ],
        name="analysis",
        compiler_params=LIMIT,
    )(meta, state, near_y, far_y, near_x, far_x, mean, anomaly)
    post_mean = jnp.transpose(post_mean, (1, 0, 2))
    post_anom = jnp.transpose(post_anom, (1, 0, 2))
    return post_mean[None], post_anom[None, None]


def solution(mesh):
    in_specs = (
        P("gx", "gy", None, None, None),
        P("gx", "gy", None, None),
        P("gx", "gy", None, None, None),
        P("gx", "gy", None),
        P("gx", "gy", None),
        P("gx", "gy", None),
        P("gx", "gy", None),
        P("gx", "gy", None),
        P("gx", "gy", None),
    )
    out_specs = (P("gx", "gy", None, None), P("gx", "gy", None, None, None))
    return jax.shard_map(local, mesh=mesh, in_specs=in_specs, out_specs=out_specs, check_vma=False)
```

```python
import jax
import jax.numpy as jnp
from jax import lax
from jax.experimental import pallas as pl
from jax.experimental.pallas import tpu as pltpu
from jax.sharding import PartitionSpec as P

MEM = 80
AX = 8
AY = 16
OCN_DEV = 1024
OB = 32
NB = 2
K = 4
FIELDS = 12
COMP = 13
CELLS = 128
OBS_DEV = 64

f32 = jnp.float32
RECORD = 3
TAPER = {0: 1.0, 1: 0.5625, 2: 0.25}
OFFSETS = [(dx, dy) for dx in (-1, 0, 1) for dy in (-1, 0, 1)]


def exchange(block, axis, first):
    count_x, count_y = lax.axis_size("gx"), lax.axis_size("gy")
    pairs = []
    for x in range(count_x):
        for y in range(count_y):
            at, count = (x, count_x) if axis == "gx" else (y, count_y)
            other = at ^ 1 if first == 0 else at - 1 + 2 * (at % 2)
            if not 0 <= other < count:
                to = (x, y ^ 1) if axis == "gx" else (x ^ 1, y)
            else:
                to = (other, y) if axis == "gx" else (x, other)
            pairs.append((x * count_y + y, to[0] * count_y + to[1]))
    return lax.ppermute(block, ("gx", "gy"), pairs)


def lanes(rows=1):
    return lax.broadcasted_iota(jnp.int32, (rows, CELLS), 1)


def records_kernel(first_hbm, w_ref, order_ref, cell_ref, live_ref, value_ref, error_ref, meta_ref):
    order = jnp.transpose(jnp.broadcast_to(order_ref[...], (OBS_DEV, OBS_DEV)))
    taken = order == lax.broadcasted_iota(jnp.int32, (OBS_DEV, OBS_DEV), 1)
    lane = lanes(8)
    records = jnp.zeros((8, CELLS), f32)
    cell = jnp.where(live_ref[...] > 0, cell_ref[...], -1).astype(f32)
    for n, row in enumerate((cell, value_ref[...], error_ref[...])):
        picked = jnp.sum(jnp.where(taken, row, 0.0), axis=1, keepdims=True)
        for g in range(OBS_DEV // 8):
            column = jnp.broadcast_to(picked[8 * g : 8 * g + 8], (8, CELLS))
            records = jnp.where(lane == RECORD * g + n, column, records)
    meta_ref[...] = records


def fields_kernel(state_hbm, atm_ref, anom_ref, mean_ref):
    mean_ref[...] = jnp.zeros_like(mean_ref)
    for v in range(FIELDS):
        field = atm_ref[v]
        mean = jnp.sum(field, axis=0, keepdims=True) / MEM
        mean_ref[v : v + 1, :] = mean
        anom_ref[v] = field - mean


def even(axis):
    return lax.axis_index(axis) % 2 == 0


def remap_kernel(slot_ref, meta_ref, w_ref, *refs):
    tiles, (state_ref, near_ref, far_ref) = refs[:9], refs[9:]
    state_ref[...] = jnp.zeros_like(state_ref)
    for index, tile in enumerate(tiles):
        k = slot_ref[index]

        @pl.when(k >= 0)
        def _(tile=tile, k=k):
            state_ref[...] += jnp.dot(tile[...], w_ref[k], preferred_element_type=f32)

    y = lanes() % AY
    high = low = jnp.zeros((16, CELLS), f32)
    for g in range(MEM // 16):
        part = state_ref[16 * g : 16 * g + 16, :]
        up = pltpu.roll(part, (CELLS - 2 * g) % CELLS, 1) if g else part
        down = pltpu.roll(part, 2 * g, 1) if g else part
        high = jnp.where(y // 2 == 7 - g, up, high)
        low = jnp.where(y // 2 == g, down, low)
    near_ref[0:16, :] = jnp.where(even("gy"), high, low)
    far_ref[0:16, :] = jnp.where(even("gy"), low, high)
    near_ref[16:24, :] = meta_ref[...]
    far_ref[16:24, :] = meta_ref[...]


def sides(near_ref, far_ref, axis):
    near, far = near_ref[...], far_ref[...]
    return jnp.where(even(axis), far, near), jnp.where(even(axis), near, far)


HALF = MEM // 2


def side_kernel(meta_ref, state_ref, near_ref, far_ref, column_ref, near_out_ref, far_out_ref):
    lane = lanes()
    before, after = sides(near_ref, far_ref, "gy")
    high_y = lane % AY >= 8
    for g in range(MEM // 16):
        lower, upper = before[0:16], after[0:16]
        if g:
            lower = pltpu.roll(lower, 2 * g, 1)
            upper = pltpu.roll(upper, CELLS - 2 * g, 1)
        column_ref[16 * g : 16 * g + 16, :] = jnp.where(high_y, lower, upper)
    quarter = lane // 32
    state_a, state_b = state_ref[0:HALF, :], state_ref[HALF:MEM, :]
    column_a, column_b = column_ref[0:HALF, :], column_ref[HALF:MEM, :]
    turned = pltpu.roll(column_a, 64, 1)

    def pack(order, blocks):
        out = blocks[3]
        for n in range(3):
            out = jnp.where(quarter == order[n], blocks[n], out)
        return out

    right = pack(
        (3, 2, 1), (state_a, pltpu.roll(state_b, 96, 1), turned, pltpu.roll(column_b, 32, 1))
    )
    left = pack(
        (0, 1, 2), (state_a, pltpu.roll(state_b, 32, 1), turned, pltpu.roll(column_b, 96, 1))
    )
    near_out_ref[0:HALF, :] = jnp.where(even("gx"), right, left)
    far_out_ref[0:HALF, :] = jnp.where(even("gx"), left, right)
    records = pack(
        (0, 1, 2),
        (
            meta_ref[...],
            pltpu.roll(before[16:24], 32, 1),
            pltpu.roll(after[16:24], 64, 1),
            jnp.zeros((8, CELLS), f32),
        ),
    )
    near_out_ref[HALF : HALF + 8, :] = records
    far_out_ref[HALF : HALF + 8, :] = records


def turned_up(a, b):
    return jnp.where(lanes() % AY == 15, pltpu.roll(b, 15, 1), pltpu.roll(a, 127, 1))


def turned_down(a, b):
    return jnp.where(lanes() % AY == 0, pltpu.roll(b, 113, 1), pltpu.roll(a, 1, 1))


def turned_right(a, b):
    return pltpu.roll(jnp.where(lanes() < AY, b, a), 112, 1)


def turned_left(a, b):
    return pltpu.roll(jnp.where(lanes() >= CELLS - AY, b, a), 16, 1)


def shifted_rows(blocks):
    m0, m1, h0, h1 = blocks
    return {
        0: blocks,
        1: [turned_up(m0, h0), turned_up(m1, h1), turned_up(h0, m0), turned_up(h1, m1)],
        -1: [turned_down(m0, h0), turned_down(m1, h1), turned_down(h0, m0), turned_down(h1, m1)],
    }


def views_of(rows, count=4):
    out = {}
    for dy, blocks in rows.items():
        out[0, dy] = list(blocks[:count])
        for dx, turn in ((1, turned_right), (-1, turned_left)):
            out[dx, dy] = [turn(blocks[n], blocks[n ^ 1]) for n in range(count)]
    return out


def own_rows(blocks):
    m0, m1, h0, h1 = blocks
    return {
        0: [m0, m1],
        1: [turned_up(m0, h0), turned_up(m1, h1)],
        -1: [turned_down(m0, h0), turned_down(m1, h1)],
    }


def own_views(blocks):
    return {key: value[0] for key, value in views_of(own_rows(blocks), 1).items()}


ROWS = MEM // 8


def group(r):
    return pl.ds(pl.multiple_of(r * 8, 8), 8)


def total(block):
    return jnp.sum(block, axis=0, keepdims=True)


def spread(rows):
    return [jnp.broadcast_to(row, (8, CELLS)) for row in rows]


def scale(key):
    return TAPER[key[0] ** 2 + key[1] ** 2] / (MEM - 1)


def present():
    at_x, at_y = lax.axis_index("gx"), lax.axis_index("gy")
    return [
        flag.astype(jnp.int32)
        for flag in (
            at_x > 0,
            at_x < lax.axis_size("gx") - 1,
            at_y > 0,
            at_y < lax.axis_size("gy") - 1,
        )
    ]


def cell_weights(record, there, batch, square, mean):
    variance = square / (MEM - 1)
    pulls = damped = jnp.zeros((8, CELLS), f32)
    for g in range(batch * OB // 8, (batch + 1) * OB // 8):
        here = (record(RECORD * g) == lanes().astype(f32)) & there
        error = record(RECORD * g + 2)
        denominator = variance + error
        pull = (record(RECORD * g + 1) - mean) / denominator
        damp = 1.0 / (denominator + jnp.sqrt(error * denominator))
        pulls = pulls + jnp.where(here, pull, 0.0)
        damped = damped + jnp.where(here, damp, 0.0)
    return total(pulls), total(damped)


def column_of(records):
    return lambda at: jnp.broadcast_to(records[:, at : at + 1], (8, CELLS))


def window_kernel(
    meta_ref, state_ref, column_ref, near_ref, far_ref, anom_ref,
    field_ref, turned_ref, rows_ref, partial_ref, view_ref,
):
    lane = lanes()
    high_y = lane % AY >= 8
    before, after = sides(near_ref, far_ref, "gy")
    lower, upper = column_of(before[16:24]), column_of(after[16:24])
    _, _, has_before, has_after = present()
    records = (
        column_of(meta_ref[...]),
        lambda at: jnp.where(high_y, lower(at), upper(at)),
    )
    there = (lane >= 0, jnp.where(high_y, has_before, has_after) > 0)
    for block, ref in enumerate((state_ref, column_ref)):
        state = ref[...]
        mean = total(state) / MEM
        anom = state - mean
        field_ref[block] = anom
        square = total(anom * anom)
        pulls, damped = cell_weights(records[block], there[block], 0, square, mean)
        rows_ref[block : block + 1, :] = mean
        rows_ref[2 + block : 3 + block, :] = pulls
        rows_ref[4 + block : 5 + block, :] = damped

    for r in range(ROWS):
        at = slice(8 * r, 8 * r + 8)
        own, beside = field_ref[0, at, :], field_ref[1, at, :]
        up, down = turned_up(own, beside), turned_down(own, beside)
        turned_ref[0, 0, at, :] = up
        turned_ref[0, 1, at, :] = turned_up(beside, own)
        turned_ref[1, 0, at, :] = down
        turned_ref[1, 1, at, :] = turned_down(beside, own)
        rows = {0: own, 1: up, -1: down}
        for n, (dx, dy) in enumerate(OFFSETS):
            view = rows[dy]
            if dx == 1:
                view = turned_right(view, 0.0)
            if dx == -1:
                view = turned_left(view, 0.0)
            view_ref[n, at, :] = view

    zero = jnp.zeros((8, CELLS), f32)
    partial_ref[...] = jnp.zeros_like(partial_ref)

    def sums_of(blocks):
        sums = [[zero] * 9 for _ in blocks]
        for r in range(ROWS):
            at = slice(8 * r, 8 * r + 8)
            shifted = [view_ref[n, at, :] for n in range(9)]
            for i, block in enumerate(blocks):
                rows = block(at)
                sums[i] = [s + rows * w for s, w in zip(sums[i], shifted)]
        return sums

    (sums,) = sums_of([lambda at: field_ref[0, at, :]])
    for n in range(9):
        partial_ref[FIELDS, n : n + 1, :] = total(sums[n])

    def pair(g, carry):
        sums = sums_of([lambda at, v=2 * g + i: anom_ref[v, at, :] for i in range(2)])
        for i in range(2):
            for n in range(9):
                partial_ref[2 * g + i, n : n + 1, :] = total(sums[i][n])
        return carry

    lax.fori_loop(0, FIELDS // 2, pair, 0)


def analysis_kernel(
    meta_ref, near_y_ref, far_y_ref, near_x_ref, far_x_ref, field_ref, turned_ref, rows_ref,
    partial_ref, mean_ref, anom_ref, post_mean_hbm, post_anom_hbm,
    other_ref, moved_ref, first_ref, edge_ref, second_ref, out_ref, out_mean_ref, sem_ref,
):
    lane = lanes()
    low_x = lane < 64
    high_y = lane % AY >= 8
    has_west, has_east, has_before, has_after = present()
    before, after = sides(near_y_ref, far_y_ref, "gy")
    west, east = sides(near_x_ref, far_x_ref, "gx")
    west_column, east_column = column_of(west[HALF:]), column_of(east[HALF:])
    lower, upper = column_of(before[16:24]), column_of(after[16:24])
    records = (
        column_of(meta_ref[...]),
        lambda at: jnp.where(low_x, east_column(at), west_column(at)),
        lambda at: jnp.where(high_y, lower(at), upper(at)),
        lambda at: jnp.where(
            low_x,
            jnp.where(high_y, east_column(32 + at), east_column(64 + at)),
            jnp.where(high_y, west_column(32 + at), west_column(64 + at)),
        ),
    )
    side_x = jnp.where(low_x, has_east, has_west)
    side_y = jnp.where(high_y, has_before, has_after)
    there = (lane >= 0, side_x > 0, side_y > 0, side_x * side_y > 0)

    means = [rows_ref[0:1, :], None, rows_ref[1:2, :], None]
    pulls = [rows_ref[2:3, :], None, rows_ref[3:4, :], None]
    damped = [rows_ref[4:5, :], None, rows_ref[5:6, :], None]
    west_half, east_half = west[0:HALF], east[0:HALF]
    halves = {
        1: (
            jnp.where(low_x, east_half, west_half),
            jnp.where(low_x, pltpu.roll(east_half, 96, 1), pltpu.roll(west_half, 32, 1)),
        ),
        3: (
            pltpu.roll(jnp.where(low_x, west_half, east_half), 64, 1),
            jnp.where(low_x, pltpu.roll(east_half, 32, 1), pltpu.roll(west_half, 96, 1)),
        ),
    }
    for block, (first, second) in halves.items():
        mean = (total(first) + total(second)) / MEM
        first, second = first - mean, second - mean
        other_ref[block // 2, 0:HALF, :] = first
        other_ref[block // 2, HALF:MEM, :] = second
        square = total(first * first) + total(second * second)
        means[block] = mean
        pulls[block], damped[block] = cell_weights(records[block], there[block], 0, square, mean)

    zero = jnp.zeros((8, CELLS), f32)
    pull_views = views_of(shifted_rows(spread(pulls)))
    damp_views = views_of(shifted_rows(spread(damped)))
    edges = [(1, dy) for dy in (-1, 0, 1)]

    def at_edge(right, left):
        return jnp.where(lane >= CELLS - AY, right, jnp.where(lane < AY, left, 0.0))

    def shift_first(r, sums):
        at = group(r)
        m0, h0 = field_ref[0, at, :], field_ref[1, at, :]
        m1, h1 = other_ref[0, at, :], other_ref[1, at, :]
        rows = {
            0: [m0, m1, h0, h1],
            1: [turned_ref[0, 0, at, :], turned_up(m1, h1), turned_ref[0, 1, at, :], turned_up(h1, m1)],
            -1: [
                turned_ref[1, 0, at, :], turned_down(m1, h1), turned_ref[1, 1, at, :], turned_down(h1, m1),
            ],
        }
        shifted = views_of(rows)
        out = []
        for n, key in enumerate(OFFSETS):
            for block in range(4):
                first_ref[block, n, at, :] = shifted[key][block]
        for n, key in enumerate(OFFSETS):
            for block in range(1, 4):
                out.append(sums[n * 3 + block - 1] + shifted[key][block] * rows[0][block])
        for n, (_, dy) in enumerate(edges):
            edge = at_edge(shifted[1, dy][0], shifted[-1, dy][0])
            edge_ref[n, at, :] = edge
            out.append(sums[27 + n] + edge * m0)
        return tuple(out)

    sums = lax.fori_loop(0, ROWS, shift_first, (zero,) * 30, unroll=2)

    def completed(v, extra):
        out = {}
        for n, key in enumerate(OFFSETS):
            covariance = partial_ref[v, n : n + 1, :]
            if key[0]:
                more = total(extra[key[1] + 1])
                covariance = covariance + jnp.where(
                    lane >= CELLS - AY if key[0] == 1 else lane < AY, more, 0.0
                )
            out[key] = covariance * scale(key)
        return out

    next_means, next_squares = [], []
    for block in range(4):
        if block == 0:
            covariances = completed(FIELDS, sums[27:30])
        else:
            covariances = {
                key: total(sums[n * 3 + block - 1]) * scale(key) for n, key in enumerate(OFFSETS)
            }
        step = jnp.zeros_like(means[block])
        gains = []
        for key in OFFSETS:
            step = step + covariances[key] * pull_views[key][block][0:1]
            gains.append(covariances[key] * damp_views[key][block][0:1])
        square = zero
        for r in range(ROWS):
            at = slice(8 * r, 8 * r + 8)
            source = other_ref if block % 2 else field_ref
            moved = source[block // 2, at, :]
            for n in range(9):
                moved = moved - gains[n] * first_ref[block, n, at, :]
            moved_ref[block, at, :] = moved
            square = square + moved * moved
        next_means.append(means[block] + step)
        next_squares.append(total(square))
    next_pulls, next_damped = [], []
    for block in range(4):
        pull, damp = cell_weights(
            records[block], there[block], 1, next_squares[block], next_means[block]
        )
        next_pulls.append(pull)
        next_damped.append(damp)
    next_pull_views = own_views(spread(next_pulls))
    next_damp_views = own_views(spread(next_damped))

    def shift_second(r, sums):
        at = group(r)
        blocks = [moved_ref[block, at, :] for block in range(4)]
        shifted = own_views(blocks)
        out = []
        for n, key in enumerate(OFFSETS):
            second_ref[n, at, :] = shifted[key]
            out.append(sums[n] + shifted[key] * blocks[0])
        return tuple(out)

    sums = lax.fori_loop(0, ROWS, shift_second, (zero,) * 9, unroll=2)

    def finish(sums, mean):
        gains = []
        for n, key in enumerate(OFFSETS):
            covariance = total(sums[n]) * scale(key)
            mean = mean + covariance * next_pull_views[key][0:1]
            gains.append(covariance * next_damp_views[key][0:1])
        return gains, mean

    gains, mean = finish(sums, next_means[0])
    out_mean_ref[FIELDS] = mean
    for r in range(ROWS):
        at = slice(8 * r, 8 * r + 8)
        block = moved_ref[0, at, :]
        for n in range(9):
            block = block - gains[n] * second_ref[n, at, :]
        out_ref[FIELDS, at, :] = block

    def send(v, count):
        return pltpu.make_async_copy(
            out_ref.at[pl.ds(v, count)], post_anom_hbm.at[pl.ds(v, count)], sem_ref.at[0]
        )

    def pair(g, carry):
        comps = [2 * g, 2 * g + 1]
        sums = [[zero] * 3, [zero] * 3]
        for r in range(ROWS):
            at = slice(8 * r, 8 * r + 8)
            shifted = [edge_ref[n, at, :] for n in range(3)]
            for i, v in enumerate(comps):
                block = anom_ref[v, at, :]
                sums[i] = [s + block * w for s, w in zip(sums[i], shifted)]
        means, gains = [], []
        for i, v in enumerate(comps):
            mean = mean_ref[pl.ds(v, 1), :]
            own = []
            for key, covariance in completed(v, sums[i]).items():
                mean = mean + covariance * pull_views[key][0][0:1]
                own.append(covariance * damp_views[key][0][0:1])
            means.append(mean)
            gains.append(own)
        sums = [[zero] * 9, [zero] * 9]
        for r in range(ROWS):
            at = slice(8 * r, 8 * r + 8)
            shifted = [first_ref[0, n, at, :] for n in range(9)]
            later = [second_ref[n, at, :] for n in range(9)]
            for i, v in enumerate(comps):
                block = anom_ref[v, at, :]
                for n in range(9):
                    block = block - gains[i][n] * shifted[n]
                out_ref[v, at, :] = block
                sums[i] = [s + block * w for s, w in zip(sums[i], later)]
        for i, v in enumerate(comps):
            gains[i], mean = finish(sums[i], means[i])
            out_mean_ref[v] = mean
        for r in range(ROWS):
            at = slice(8 * r, 8 * r + 8)
            later = [second_ref[n, at, :] for n in range(9)]
            for i, v in enumerate(comps):
                block = out_ref[v, at, :]
                for n in range(9):
                    block = block - gains[i][n] * later[n]
                out_ref[v, at, :] = block
        send(2 * g, 2).start()
        return carry

    send(FIELDS, 1).start()
    lax.fori_loop(0, FIELDS // 2, pair, 0)
    last = pltpu.make_async_copy(out_mean_ref, post_mean_hbm, sem_ref.at[1])
    last.start()
    pltpu.make_async_copy(out_ref, post_anom_hbm, sem_ref.at[0]).wait()
    last.wait()


VMEM = pl.BlockSpec(memory_space=pltpu.VMEM)
SMEM = pl.BlockSpec(memory_space=pltpu.SMEM)
ANY = pl.BlockSpec(memory_space=pl.ANY)
LIMIT = pltpu.CompilerParams(vmem_limit_bytes=8 << 20)


def flat(*shape):
    return jax.ShapeDtypeStruct(shape, f32)


def local(
    atm_members,
    ocean_members,
    remap_weights,
    pair_src,
    obs_cell,
    obs_value,
    obs_error,
    obs_live,
    obs_order,
):
    at_x = lax.axis_index("gx")
    at_y = lax.axis_index("gy")
    rows = lax.axis_size("gy")
    own = ocean_members[0, 0]
    column = [own] + [exchange(own, "gy", first) for first in (0, 1)]
    tiles = list(column)
    for first in (0, 1):
        tiles += [exchange(tile, "gx", first) for tile in column]
    source = pair_src[0, 0]

    def slot(step, at):
        return jnp.where(step == 0, 0, jnp.where((step == 1) == (at % 2 == 0), 1, 2))

    select = slot(source // rows - at_x, at_x) * 3 + slot(source % rows - at_y, at_y)
    listed = select[None, :] == jnp.arange(9, dtype=jnp.int32)[:, None]
    slots = jnp.max(jnp.where(listed, jnp.arange(K, dtype=jnp.int32)[None, :], -1), axis=1)
    weights = remap_weights[0, 0]
    meta = pl.pallas_call(
        records_kernel,
        in_specs=[ANY] + [VMEM] * 6,
        out_specs=VMEM,
        out_shape=flat(8, CELLS),
        name="records",
        compiler_params=LIMIT,
    )(column[2], weights, obs_order[0], obs_cell[0], obs_live[0], obs_value[0], obs_error[0])
    state, near_message, far_message = pl.pallas_call(
        remap_kernel,
        in_specs=[SMEM, VMEM, VMEM] + [VMEM] * 9,
        out_specs=[VMEM] * 3,
        out_shape=[flat(MEM, CELLS), flat(24, CELLS), flat(24, CELLS)],
        name="remap",
        compiler_params=LIMIT,
    )(slots, meta, weights, *tiles)
    near_y = exchange(near_message, "gy", 0)
    far_y = exchange(far_message, "gy", 1)
    anomaly, mean = pl.pallas_call(
        fields_kernel,
        in_specs=[ANY, VMEM],
        out_specs=[VMEM, VMEM],
        out_shape=[flat(FIELDS, MEM, CELLS), flat(16, CELLS)],
        name="fields",
        compiler_params=LIMIT,
    )(state, jnp.transpose(atm_members[0, 0], (1, 0, 2)))
    beside, near_out, far_out = pl.pallas_call(
        side_kernel,
        in_specs=[VMEM] * 4,
        out_specs=[VMEM] * 3,
        out_shape=[flat(MEM, CELLS), flat(HALF + 8, CELLS), flat(HALF + 8, CELLS)],
        name="side",
        compiler_params=LIMIT,
    )(meta, state, near_y, far_y)
    near_x = exchange(near_out, "gx", 0)
    far_x = exchange(far_out, "gx", 1)
    field, turned, rows, partial = pl.pallas_call(
        window_kernel,
        in_specs=[VMEM] * 6,
        out_specs=[VMEM] * 4,
        out_shape=[
            flat(2, MEM, CELLS),
            flat(2, 2, MEM, CELLS),
            flat(8, CELLS),
            flat(COMP, 16, CELLS),
        ],
        scratch_shapes=[pltpu.VMEM((9, MEM, CELLS), f32)],
        name="window",
        compiler_params=LIMIT,
    )(meta, state, beside, near_y, far_y, anomaly)
    post_mean, post_anom = pl.pallas_call(
        analysis_kernel,
        in_specs=[VMEM] * 11,
        out_specs=[ANY, ANY],
        out_shape=[flat(COMP, 1, CELLS), flat(COMP, MEM, CELLS)],
        scratch_shapes=[
            pltpu.VMEM((2, MEM, CELLS), f32),
            pltpu.VMEM((4, MEM, CELLS), f32),
            pltpu.VMEM((4, 9, MEM, CELLS), f32),
            pltpu.VMEM((3, MEM, CELLS), f32),
            pltpu.VMEM((9, MEM, CELLS), f32),
            pltpu.VMEM((COMP, MEM, CELLS), f32),
            pltpu.VMEM((COMP, 1, CELLS), f32),
            pltpu.SemaphoreType.DMA((2,)),
        ],
        name="analysis",
        compiler_params=LIMIT,
    )(meta, near_y, far_y, near_x, far_x, field, turned, rows, partial, mean, anomaly)
    post_mean = jnp.transpose(post_mean, (1, 0, 2))
    post_anom = jnp.transpose(post_anom, (1, 0, 2))
    return post_mean[None], post_anom[None, None]


def solution(mesh):
    in_specs = (
        P("gx", "gy", None, None, None),
        P("gx", "gy", None, None),
        P("gx", "gy", None, None, None),
        P("gx", "gy", None),
        P("gx", "gy", None),
        P("gx", "gy", None),
        P("gx", "gy", None),
        P("gx", "gy", None),
        P("gx", "gy", None),
    )
    out_specs = (P("gx", "gy", None, None), P("gx", "gy", None, None, None))
    return jax.shard_map(local, mesh=mesh, in_specs=in_specs, out_specs=out_specs, check_vma=False)
```

```python
import jax
import jax.numpy as jnp
from jax import lax
from jax.experimental import pallas as pl
from jax.experimental.pallas import tpu as pltpu
from jax.sharding import PartitionSpec as P


MEM = 80
AY = 16
OB = 32
K = 4
FIELDS = 12
COMP = 13
CELLS = 128
OBS_DEV = 64

f32 = jnp.float32
RECORD = 3
TAPER = {0: 1.0, 1: 0.5625, 2: 0.25}
OFFSETS = [(dx, dy) for dx in (-1, 0, 1) for dy in (-1, 0, 1)]


def exchange(block, axis, first):
    count_x, count_y = lax.axis_size("gx"), lax.axis_size("gy")
    pairs = []
    for x in range(count_x):
        for y in range(count_y):
            at, count = (x, count_x) if axis == "gx" else (y, count_y)
            other = at ^ 1 if first == 0 else at - 1 + 2 * (at % 2)
            if not 0 <= other < count:
                to = (x, y ^ 1) if axis == "gx" else (x ^ 1, y)
            else:
                to = (other, y) if axis == "gx" else (x, other)
            pairs.append((x * count_y + y, to[0] * count_y + to[1]))
    return lax.ppermute(block, ("gx", "gy"), pairs)


def lanes(rows=1):
    return lax.broadcasted_iota(jnp.int32, (rows, CELLS), 1)


def records_kernel(first_hbm, w_ref, order_ref, cell_ref, live_ref, value_ref, error_ref, meta_ref):
    order = jnp.transpose(jnp.broadcast_to(order_ref[...], (OBS_DEV, OBS_DEV)))
    taken = order == lax.broadcasted_iota(jnp.int32, (OBS_DEV, OBS_DEV), 1)
    lane = lanes(8)
    records = jnp.zeros((8, CELLS), f32)
    cell = jnp.where(live_ref[...] > 0, cell_ref[...], -1).astype(f32)
    for n, row in enumerate((cell, value_ref[...], error_ref[...])):
        picked = jnp.sum(jnp.where(taken, row, 0.0), axis=1, keepdims=True)
        for g in range(OBS_DEV // 8):
            column = jnp.broadcast_to(picked[8 * g : 8 * g + 8], (8, CELLS))
            records = jnp.where(lane == RECORD * g + n, column, records)
    meta_ref[...] = records


def fields_kernel(state_hbm, atm_ref, anom_ref, mean_ref):
    mean_ref[...] = jnp.zeros_like(mean_ref)
    for v in range(FIELDS):
        field = atm_ref[v]
        mean = jnp.sum(field, axis=0, keepdims=True) / MEM
        mean_ref[v : v + 1, :] = mean
        anom_ref[v] = field - mean


def even(axis):
    return lax.axis_index(axis) % 2 == 0


def remap_kernel(slot_ref, meta_ref, w_ref, *refs):
    tiles, (state_ref, near_ref, far_ref) = refs[:9], refs[9:]
    state_ref[...] = jnp.zeros_like(state_ref)
    for index, tile in enumerate(tiles):
        k = slot_ref[index]

        @pl.when(k >= 0)
        def _(tile=tile, k=k):
            state_ref[...] += jnp.dot(tile[...], w_ref[k], preferred_element_type=f32)

    y = lanes() % AY
    high = low = jnp.zeros((16, CELLS), f32)
    for g in range(MEM // 16):
        part = state_ref[16 * g : 16 * g + 16, :]
        up = pltpu.roll(part, (CELLS - 2 * g) % CELLS, 1) if g else part
        down = pltpu.roll(part, 2 * g, 1) if g else part
        high = jnp.where(y // 2 == 7 - g, up, high)
        low = jnp.where(y // 2 == g, down, low)
    near_ref[0:16, :] = jnp.where(even("gy"), high, low)
    far_ref[0:16, :] = jnp.where(even("gy"), low, high)
    near_ref[16:24, :] = meta_ref[...]
    far_ref[16:24, :] = meta_ref[...]


def sides(near_ref, far_ref, axis):
    near, far = near_ref[...], far_ref[...]
    return jnp.where(even(axis), far, near), jnp.where(even(axis), near, far)


HALF = MEM // 2


def side_kernel(meta_ref, state_ref, near_ref, far_ref, column_ref, near_out_ref, far_out_ref):
    lane = lanes()
    before, after = sides(near_ref, far_ref, "gy")
    high_y = lane % AY >= 8
    for g in range(MEM // 16):
        lower, upper = before[0:16], after[0:16]
        if g:
            lower = pltpu.roll(lower, 2 * g, 1)
            upper = pltpu.roll(upper, CELLS - 2 * g, 1)
        column_ref[16 * g : 16 * g + 16, :] = jnp.where(high_y, lower, upper)
    quarter = lane // 32
    state_a, state_b = state_ref[0:HALF, :], state_ref[HALF:MEM, :]
    column_a, column_b = column_ref[0:HALF, :], column_ref[HALF:MEM, :]
    turned = pltpu.roll(column_a, 64, 1)

    def pack(order, blocks):
        out = blocks[3]
        for n in range(3):
            out = jnp.where(quarter == order[n], blocks[n], out)
        return out

    right = pack(
        (3, 2, 1), (state_a, pltpu.roll(state_b, 96, 1), turned, pltpu.roll(column_b, 32, 1))
    )
    left = pack(
        (0, 1, 2), (state_a, pltpu.roll(state_b, 32, 1), turned, pltpu.roll(column_b, 96, 1))
    )
    near_out_ref[0:HALF, :] = jnp.where(even("gx"), right, left)
    far_out_ref[0:HALF, :] = jnp.where(even("gx"), left, right)
    records = pack(
        (0, 1, 2),
        (
            meta_ref[...],
            pltpu.roll(before[16:24], 32, 1),
            pltpu.roll(after[16:24], 64, 1),
            jnp.zeros((8, CELLS), f32),
        ),
    )
    near_out_ref[HALF : HALF + 8, :] = records
    far_out_ref[HALF : HALF + 8, :] = records


def turned_up(a, b):
    return jnp.where(lanes() % AY == 15, pltpu.roll(b, 15, 1), pltpu.roll(a, 127, 1))


def turned_down(a, b):
    return jnp.where(lanes() % AY == 0, pltpu.roll(b, 113, 1), pltpu.roll(a, 1, 1))


def turned_right(a, b):
    return pltpu.roll(jnp.where(lanes() < AY, b, a), 112, 1)


def turned_left(a, b):
    return pltpu.roll(jnp.where(lanes() >= CELLS - AY, b, a), 16, 1)


def shifted_rows(blocks):
    m0, m1, h0, h1 = blocks
    return {
        0: blocks,
        1: [turned_up(m0, h0), turned_up(m1, h1), turned_up(h0, m0), turned_up(h1, m1)],
        -1: [turned_down(m0, h0), turned_down(m1, h1), turned_down(h0, m0), turned_down(h1, m1)],
    }


def views_of(rows, count=4):
    out = {}
    for dy, blocks in rows.items():
        out[0, dy] = list(blocks[:count])
        for dx, turn in ((1, turned_right), (-1, turned_left)):
            out[dx, dy] = [turn(blocks[n], blocks[n ^ 1]) for n in range(count)]
    return out


def own_rows(blocks):
    m0, m1, h0, h1 = blocks
    return {
        0: [m0, m1],
        1: [turned_up(m0, h0), turned_up(m1, h1)],
        -1: [turned_down(m0, h0), turned_down(m1, h1)],
    }


def own_views(blocks):
    return {key: value[0] for key, value in views_of(own_rows(blocks), 1).items()}


ROWS = MEM // 8


def group(r):
    return pl.ds(pl.multiple_of(r * 8, 8), 8)


def total(block):
    return jnp.sum(block, axis=0, keepdims=True)


def spread(rows):
    return [jnp.broadcast_to(row, (8, CELLS)) for row in rows]


def scale(key):
    return TAPER[key[0] ** 2 + key[1] ** 2] / (MEM - 1)


def present():
    at_x, at_y = lax.axis_index("gx"), lax.axis_index("gy")
    return [
        flag.astype(jnp.int32)
        for flag in (
            at_x > 0,
            at_x < lax.axis_size("gx") - 1,
            at_y > 0,
            at_y < lax.axis_size("gy") - 1,
        )
    ]


def cell_weights(record, there, batch, square, mean):
    variance = square / (MEM - 1)
    pulls = damped = jnp.zeros((8, CELLS), f32)
    for g in range(batch * OB // 8, (batch + 1) * OB // 8):
        here = (record(RECORD * g) == lanes().astype(f32)) & there
        error = record(RECORD * g + 2)
        denominator = variance + error
        pull = (record(RECORD * g + 1) - mean) / denominator
        damp = 1.0 / (denominator + jnp.sqrt(error * denominator))
        pulls = pulls + jnp.where(here, pull, 0.0)
        damped = damped + jnp.where(here, damp, 0.0)
    return total(pulls), total(damped)


def column_of(records):
    return lambda at: jnp.broadcast_to(records[:, at : at + 1], (8, CELLS))


def window_kernel(
    meta_ref, state_ref, column_ref, near_ref, far_ref, anom_ref,
    field_ref, turned_ref, rows_ref, partial_ref, view_ref,
):
    lane = lanes()
    high_y = lane % AY >= 8
    before, after = sides(near_ref, far_ref, "gy")
    lower, upper = column_of(before[16:24]), column_of(after[16:24])
    _, _, has_before, has_after = present()
    records = (
        column_of(meta_ref[...]),
        lambda at: jnp.where(high_y, lower(at), upper(at)),
    )
    there = (lane >= 0, jnp.where(high_y, has_before, has_after) > 0)
    for block, ref in enumerate((state_ref, column_ref)):
        state = ref[...]
        mean = total(state) / MEM
        anom = state - mean
        field_ref[block] = anom
        square = total(anom * anom)
        pulls, damped = cell_weights(records[block], there[block], 0, square, mean)
        rows_ref[block : block + 1, :] = mean
        rows_ref[2 + block : 3 + block, :] = pulls
        rows_ref[4 + block : 5 + block, :] = damped

    for r in range(ROWS):
        at = slice(8 * r, 8 * r + 8)
        own, beside = field_ref[0, at, :], field_ref[1, at, :]
        up, down = turned_up(own, beside), turned_down(own, beside)
        turned_ref[0, 0, at, :] = up
        turned_ref[0, 1, at, :] = turned_up(beside, own)
        turned_ref[1, 0, at, :] = down
        turned_ref[1, 1, at, :] = turned_down(beside, own)
        rows = {0: own, 1: up, -1: down}
        for n, (dx, dy) in enumerate(OFFSETS):
            view = rows[dy]
            if dx == 1:
                view = turned_right(view, 0.0)
            if dx == -1:
                view = turned_left(view, 0.0)
            view_ref[n, at, :] = view

    zero = jnp.zeros((8, CELLS), f32)
    partial_ref[...] = jnp.zeros_like(partial_ref)

    def sums_of(blocks):
        sums = [[zero] * 9 for _ in blocks]
        for r in range(ROWS):
            at = slice(8 * r, 8 * r + 8)
            shifted = [view_ref[n, at, :] for n in range(9)]
            for i, block in enumerate(blocks):
                rows = block(at)
                sums[i] = [s + rows * w for s, w in zip(sums[i], shifted)]
        return sums

    (sums,) = sums_of([lambda at: field_ref[0, at, :]])
    for n in range(9):
        partial_ref[FIELDS, n : n + 1, :] = total(sums[n])

    def pair(g, carry):
        sums = sums_of([lambda at, v=2 * g + i: anom_ref[v, at, :] for i in range(2)])
        for i in range(2):
            for n in range(9):
                partial_ref[2 * g + i, n : n + 1, :] = total(sums[i][n])
        return carry

    lax.fori_loop(0, FIELDS // 2, pair, 0)


def analysis_kernel(
    meta_ref, near_y_ref, far_y_ref, near_x_ref, far_x_ref, field_ref, turned_ref, rows_ref,
    partial_ref, mean_ref, anom_ref, post_mean_hbm, post_anom_hbm,
    other_ref, moved_ref, first_ref, edge_ref, second_ref, out_ref, out_mean_ref, sem_ref,
):
    lane = lanes()
    low_x = lane < 64
    high_y = lane % AY >= 8
    has_west, has_east, has_before, has_after = present()
    before, after = sides(near_y_ref, far_y_ref, "gy")
    west, east = sides(near_x_ref, far_x_ref, "gx")
    west_column, east_column = column_of(west[HALF:]), column_of(east[HALF:])
    lower, upper = column_of(before[16:24]), column_of(after[16:24])
    records = (
        column_of(meta_ref[...]),
        lambda at: jnp.where(low_x, east_column(at), west_column(at)),
        lambda at: jnp.where(high_y, lower(at), upper(at)),
        lambda at: jnp.where(
            low_x,
            jnp.where(high_y, east_column(32 + at), east_column(64 + at)),
            jnp.where(high_y, west_column(32 + at), west_column(64 + at)),
        ),
    )
    side_x = jnp.where(low_x, has_east, has_west)
    side_y = jnp.where(high_y, has_before, has_after)
    there = (lane >= 0, side_x > 0, side_y > 0, side_x * side_y > 0)

    means = [rows_ref[0:1, :], None, rows_ref[1:2, :], None]
    pulls = [rows_ref[2:3, :], None, rows_ref[3:4, :], None]
    damped = [rows_ref[4:5, :], None, rows_ref[5:6, :], None]
    west_half, east_half = west[0:HALF], east[0:HALF]
    halves = {
        1: (
            jnp.where(low_x, east_half, west_half),
            jnp.where(low_x, pltpu.roll(east_half, 96, 1), pltpu.roll(west_half, 32, 1)),
        ),
        3: (
            pltpu.roll(jnp.where(low_x, west_half, east_half), 64, 1),
            jnp.where(low_x, pltpu.roll(east_half, 32, 1), pltpu.roll(west_half, 96, 1)),
        ),
    }
    for block, (first, second) in halves.items():
        mean = (total(first) + total(second)) / MEM
        first, second = first - mean, second - mean
        other_ref[block // 2, 0:HALF, :] = first
        other_ref[block // 2, HALF:MEM, :] = second
        square = total(first * first) + total(second * second)
        means[block] = mean
        pulls[block], damped[block] = cell_weights(records[block], there[block], 0, square, mean)

    zero = jnp.zeros((8, CELLS), f32)
    pull_views = views_of(shifted_rows(spread(pulls)))
    damp_views = views_of(shifted_rows(spread(damped)))
    edges = [(1, dy) for dy in (-1, 0, 1)]

    def at_edge(right, left):
        return jnp.where(lane >= CELLS - AY, right, jnp.where(lane < AY, left, 0.0))

    def shift_first(r, sums):
        at = group(r)
        m0, h0 = field_ref[0, at, :], field_ref[1, at, :]
        m1, h1 = other_ref[0, at, :], other_ref[1, at, :]
        rows = {
            0: [m0, m1, h0, h1],
            1: [turned_ref[0, 0, at, :], turned_up(m1, h1), turned_ref[0, 1, at, :], turned_up(h1, m1)],
            -1: [
                turned_ref[1, 0, at, :], turned_down(m1, h1), turned_ref[1, 1, at, :], turned_down(h1, m1),
            ],
        }
        shifted = views_of(rows)
        out = []
        for n, key in enumerate(OFFSETS):
            for block in range(4):
                first_ref[block, n, at, :] = shifted[key][block]
        for n, key in enumerate(OFFSETS):
            for block in range(1, 4):
                out.append(sums[n * 3 + block - 1] + shifted[key][block] * rows[0][block])
        for n, (_, dy) in enumerate(edges):
            edge = at_edge(shifted[1, dy][0], shifted[-1, dy][0])
            edge_ref[n, at, :] = edge
            out.append(sums[27 + n] + edge * m0)
        return tuple(out)

    sums = lax.fori_loop(0, ROWS, shift_first, (zero,) * 30, unroll=5)

    def completed(v, extra):
        out = {}
        for n, key in enumerate(OFFSETS):
            covariance = partial_ref[v, n : n + 1, :]
            if key[0]:
                more = total(extra[key[1] + 1])
                covariance = covariance + jnp.where(
                    lane >= CELLS - AY if key[0] == 1 else lane < AY, more, 0.0
                )
            out[key] = covariance * scale(key)
        return out

    next_means, next_squares = [], []
    for block in range(4):
        if block == 0:
            covariances = completed(FIELDS, sums[27:30])
        else:
            covariances = {
                key: total(sums[n * 3 + block - 1]) * scale(key) for n, key in enumerate(OFFSETS)
            }
        step = jnp.zeros_like(means[block])
        gains = []
        for key in OFFSETS:
            step = step + covariances[key] * pull_views[key][block][0:1]
            gains.append(covariances[key] * damp_views[key][block][0:1])
        square = zero
        for r in range(ROWS):
            at = slice(8 * r, 8 * r + 8)
            source = other_ref if block % 2 else field_ref
            moved = source[block // 2, at, :]
            for n in range(9):
                moved = moved - gains[n] * first_ref[block, n, at, :]
            moved_ref[block, at, :] = moved
            square = square + moved * moved
        next_means.append(means[block] + step)
        next_squares.append(total(square))
    next_pulls, next_damped = [], []
    for block in range(4):
        pull, damp = cell_weights(
            records[block], there[block], 1, next_squares[block], next_means[block]
        )
        next_pulls.append(pull)
        next_damped.append(damp)
    next_pull_views = own_views(spread(next_pulls))
    next_damp_views = own_views(spread(next_damped))

    def shift_second(r, sums):
        at = group(r)
        blocks = [moved_ref[block, at, :] for block in range(4)]
        shifted = own_views(blocks)
        out = []
        for n, key in enumerate(OFFSETS):
            second_ref[n, at, :] = shifted[key]
            out.append(sums[n] + shifted[key] * blocks[0])
        return tuple(out)

    sums = lax.fori_loop(0, ROWS, shift_second, (zero,) * 9, unroll=5)

    def finish(sums, mean):
        gains = []
        for n, key in enumerate(OFFSETS):
            covariance = total(sums[n]) * scale(key)
            mean = mean + covariance * next_pull_views[key][0:1]
            gains.append(covariance * next_damp_views[key][0:1])
        return gains, mean

    gains, mean = finish(sums, next_means[0])
    out_mean_ref[FIELDS] = mean
    for r in range(ROWS):
        at = slice(8 * r, 8 * r + 8)
        block = moved_ref[0, at, :]
        for n in range(9):
            block = block - gains[n] * second_ref[n, at, :]
        out_ref[FIELDS, at, :] = block

    def send(v, count):
        return pltpu.make_async_copy(
            out_ref.at[pl.ds(v, count)], post_anom_hbm.at[pl.ds(v, count)], sem_ref.at[0]
        )

    def pair(g, carry):
        comps = [2 * g, 2 * g + 1]
        sums = [[zero] * 3, [zero] * 3]
        for r in range(ROWS):
            at = slice(8 * r, 8 * r + 8)
            shifted = [edge_ref[n, at, :] for n in range(3)]
            for i, v in enumerate(comps):
                block = anom_ref[v, at, :]
                sums[i] = [s + block * w for s, w in zip(sums[i], shifted)]
        means, gains = [], []
        for i, v in enumerate(comps):
            mean = mean_ref[pl.ds(v, 1), :]
            own = []
            for key, covariance in completed(v, sums[i]).items():
                mean = mean + covariance * pull_views[key][0][0:1]
                own.append(covariance * damp_views[key][0][0:1])
            means.append(mean)
            gains.append(own)
        sums = [[zero] * 9, [zero] * 9]
        for r in range(ROWS):
            at = slice(8 * r, 8 * r + 8)
            shifted = [first_ref[0, n, at, :] for n in range(9)]
            later = [second_ref[n, at, :] for n in range(9)]
            for i, v in enumerate(comps):
                block = anom_ref[v, at, :]
                for n in range(9):
                    block = block - gains[i][n] * shifted[n]
                out_ref[v, at, :] = block
                sums[i] = [s + block * w for s, w in zip(sums[i], later)]
        for i, v in enumerate(comps):
            gains[i], mean = finish(sums[i], means[i])
            out_mean_ref[v] = mean
        for r in range(ROWS):
            at = slice(8 * r, 8 * r + 8)
            later = [second_ref[n, at, :] for n in range(9)]
            for i, v in enumerate(comps):
                block = out_ref[v, at, :]
                for n in range(9):
                    block = block - gains[i][n] * later[n]
                out_ref[v, at, :] = block
        send(2 * g, 2).start()
        return carry

    send(FIELDS, 1).start()
    lax.fori_loop(0, FIELDS // 2, pair, 0)
    last = pltpu.make_async_copy(out_mean_ref, post_mean_hbm, sem_ref.at[1])
    last.start()
    pltpu.make_async_copy(out_ref, post_anom_hbm, sem_ref.at[0]).wait()
    last.wait()


VMEM = pl.BlockSpec(memory_space=pltpu.VMEM)
SMEM = pl.BlockSpec(memory_space=pltpu.SMEM)
ANY = pl.BlockSpec(memory_space=pl.ANY)
LIMIT = pltpu.CompilerParams(vmem_limit_bytes=8 << 20)


def flat(*shape):
    return jax.ShapeDtypeStruct(shape, f32)


def local(
    atm_members,
    ocean_members,
    remap_weights,
    pair_src,
    obs_cell,
    obs_value,
    obs_error,
    obs_live,
    obs_order,
):
    at_x = lax.axis_index("gx")
    at_y = lax.axis_index("gy")
    rows = lax.axis_size("gy")
    own = ocean_members[0, 0]
    column = [own]
    for first in (0, 1):
        column.append(exchange(own, "gy", first))
    tiles = list(column)
    for first in (0, 1):
        for tile in column:
            tiles.append(exchange(tile, "gx", first))
    source = pair_src[0, 0]

    def slot(step, at):
        return jnp.where(step == 0, 0, jnp.where((step == 1) == (at % 2 == 0), 1, 2))

    select = slot(source // rows - at_x, at_x) * 3 + slot(source % rows - at_y, at_y)
    listed = select[None, :] == jnp.arange(9, dtype=jnp.int32)[:, None]
    slots = jnp.max(jnp.where(listed, jnp.arange(K, dtype=jnp.int32)[None, :], -1), axis=1)
    weights = remap_weights[0, 0]
    meta = pl.pallas_call(
        records_kernel,
        in_specs=[ANY] + [VMEM] * 6,
        out_specs=VMEM,
        out_shape=flat(8, CELLS),
        name="records",
        compiler_params=LIMIT,
    )(column[2], weights, obs_order[0], obs_cell[0], obs_live[0], obs_value[0], obs_error[0])
    state, near_message, far_message = pl.pallas_call(
        remap_kernel,
        in_specs=[SMEM, VMEM, VMEM] + [VMEM] * 9,
        out_specs=[VMEM] * 3,
        out_shape=[flat(MEM, CELLS), flat(24, CELLS), flat(24, CELLS)],
        name="remap",
        compiler_params=LIMIT,
    )(slots, meta, weights, *tiles)
    near_y = exchange(near_message, "gy", 0)
    far_y = exchange(far_message, "gy", 1)
    anomaly, mean = pl.pallas_call(
        fields_kernel,
        in_specs=[ANY, VMEM],
        out_specs=[VMEM, VMEM],
        out_shape=[flat(FIELDS, MEM, CELLS), flat(16, CELLS)],
        name="fields",
        compiler_params=LIMIT,
    )(state, jnp.transpose(atm_members[0, 0], (1, 0, 2)))
    beside, near_out, far_out = pl.pallas_call(
        side_kernel,
        in_specs=[VMEM] * 4,
        out_specs=[VMEM] * 3,
        out_shape=[flat(MEM, CELLS), flat(HALF + 8, CELLS), flat(HALF + 8, CELLS)],
        name="side",
        compiler_params=LIMIT,
    )(meta, state, near_y, far_y)
    near_x = exchange(near_out, "gx", 0)
    far_x = exchange(far_out, "gx", 1)
    field, turned, rows, partial = pl.pallas_call(
        window_kernel,
        in_specs=[VMEM] * 6,
        out_specs=[VMEM] * 4,
        out_shape=[
            flat(2, MEM, CELLS),
            flat(2, 2, MEM, CELLS),
            flat(8, CELLS),
            flat(COMP, 16, CELLS),
        ],
        scratch_shapes=[pltpu.VMEM((9, MEM, CELLS), f32)],
        name="window",
        compiler_params=LIMIT,
    )(meta, state, beside, near_y, far_y, anomaly)
    post_mean, post_anom = pl.pallas_call(
        analysis_kernel,
        in_specs=[VMEM] * 11,
        out_specs=[ANY, ANY],
        out_shape=[flat(COMP, 1, CELLS), flat(COMP, MEM, CELLS)],
        scratch_shapes=[
            pltpu.VMEM((2, MEM, CELLS), f32),
            pltpu.VMEM((4, MEM, CELLS), f32),
            pltpu.VMEM((4, 9, MEM, CELLS), f32),
            pltpu.VMEM((3, MEM, CELLS), f32),
            pltpu.VMEM((9, MEM, CELLS), f32),
            pltpu.VMEM((COMP, MEM, CELLS), f32),
            pltpu.VMEM((COMP, 1, CELLS), f32),
            pltpu.SemaphoreType.DMA((2,)),
        ],
        name="analysis",
        compiler_params=LIMIT,
    )(meta, near_y, far_y, near_x, far_x, field, turned, rows, partial, mean, anomaly)
    post_mean = jnp.transpose(post_mean, (1, 0, 2))
    post_anom = jnp.transpose(post_anom, (1, 0, 2))
    return post_mean[None], post_anom[None, None]


def solution(mesh):
    in_specs = (
        P("gx", "gy", None, None, None),
        P("gx", "gy", None, None),
        P("gx", "gy", None, None, None),
        P("gx", "gy", None),
        P("gx", "gy", None),
        P("gx", "gy", None),
        P("gx", "gy", None),
        P("gx", "gy", None),
        P("gx", "gy", None),
    )
    out_specs = (P("gx", "gy", None, None), P("gx", "gy", None, None, None))

    return jax.shard_map(local, mesh=mesh, in_specs=in_specs, out_specs=out_specs, check_vma=False)
```

```python
import jax
import jax.numpy as jnp
from jax import lax
from jax.experimental import pallas as pl
from jax.experimental.pallas import tpu as pltpu
from jax.sharding import PartitionSpec as P


MEM = 80
AY = 16
OB = 32
K = 4
FIELDS = 12
COMP = 13
CELLS = 128
OBS_DEV = 64

f32 = jnp.float32
RECORD = 3
TAPER = {0: 1.0, 1: 0.5625, 2: 0.25}
OFFSETS = [(dx, dy) for dx in (-1, 0, 1) for dy in (-1, 0, 1)]


def exchange(block, axis, first):
    count_x, count_y = lax.axis_size("gx"), lax.axis_size("gy")
    pairs = []
    for x in range(count_x):
        for y in range(count_y):
            at, count = (x, count_x) if axis == "gx" else (y, count_y)
            other = at ^ 1 if first == 0 else at - 1 + 2 * (at % 2)
            if not 0 <= other < count:
                to = (x, y ^ 1) if axis == "gx" else (x ^ 1, y)
            else:
                to = (other, y) if axis == "gx" else (x, other)
            pairs.append((x * count_y + y, to[0] * count_y + to[1]))
    return lax.ppermute(block, ("gx", "gy"), pairs)


def lanes(rows=1):
    return lax.broadcasted_iota(jnp.int32, (rows, CELLS), 1)


def records_kernel(first_hbm, slots_ref, meta_ref):
    order = jnp.transpose(jnp.broadcast_to(slots_ref[0:1, :], (OBS_DEV, OBS_DEV)))
    taken = order == lax.broadcasted_iota(jnp.int32, (OBS_DEV, OBS_DEV), 1).astype(f32)
    lane = lanes(8)
    records = jnp.zeros((8, CELLS), f32)
    for n in range(RECORD):
        row = slots_ref[n + 1 : n + 2, :]
        picked = jnp.sum(jnp.where(taken, row, 0.0), axis=1, keepdims=True)
        for g in range(OBS_DEV // 8):
            column = jnp.broadcast_to(picked[8 * g : 8 * g + 8], (8, CELLS))
            records = jnp.where(lane == RECORD * g + n, column, records)
    meta_ref[...] = records


def fields_kernel(state_hbm, atm_ref, anom_ref, mean_ref):
    mean_ref[...] = jnp.zeros_like(mean_ref)
    for v in range(FIELDS):
        field = atm_ref[v]
        mean = jnp.sum(field, axis=0, keepdims=True) / MEM
        mean_ref[v : v + 1, :] = mean
        anom_ref[v] = field - mean


def even(axis):
    return lax.axis_index(axis) % 2 == 0


def add_tiles(slot_ref, w_ref, indices, tiles, sum_ref):
    for index, tile in zip(indices, tiles):
        k = slot_ref[index]

        @pl.when(k >= 0)
        def _(tile=tile, k=k):
            sum_ref[...] += jnp.dot(tile[...], w_ref[k], preferred_element_type=f32)


EARLY = (0, 1, 2, 3, 6)
LATE = (4, 5, 7, 8)


def early_kernel(slot_ref, after_hbm, w_ref, *refs):
    tiles, sum_ref = refs[:-1], refs[-1]
    sum_ref[...] = jnp.zeros_like(sum_ref)
    add_tiles(slot_ref, w_ref, EARLY, tiles, sum_ref)


def remap_kernel(slot_ref, meta_ref, w_ref, sum_ref, *refs):
    tiles, (state_ref, near_ref, far_ref) = refs[:4], refs[4:]
    state_ref[...] = sum_ref[...]
    add_tiles(slot_ref, w_ref, LATE, tiles, state_ref)

    y = lanes() % AY
    high = low = jnp.zeros((16, CELLS), f32)
    for g in range(MEM // 16):
        part = state_ref[16 * g : 16 * g + 16, :]
        up = pltpu.roll(part, (CELLS - 2 * g) % CELLS, 1) if g else part
        down = pltpu.roll(part, 2 * g, 1) if g else part
        high = jnp.where(y // 2 == 7 - g, up, high)
        low = jnp.where(y // 2 == g, down, low)
    near_ref[0:16, :] = jnp.where(even("gy"), high, low)
    far_ref[0:16, :] = jnp.where(even("gy"), low, high)
    near_ref[16:24, :] = meta_ref[...]
    far_ref[16:24, :] = meta_ref[...]


def sides(near_ref, far_ref, axis):
    near, far = near_ref[...], far_ref[...]
    return jnp.where(even(axis), far, near), jnp.where(even(axis), near, far)


HALF = MEM // 2


def side_kernel(meta_ref, state_ref, near_ref, far_ref, column_ref, near_out_ref, far_out_ref):
    lane = lanes()
    before, after = sides(near_ref, far_ref, "gy")
    high_y = lane % AY >= 8
    for g in range(MEM // 16):
        lower, upper = before[0:16], after[0:16]
        if g:
            lower = pltpu.roll(lower, 2 * g, 1)
            upper = pltpu.roll(upper, CELLS - 2 * g, 1)
        column_ref[16 * g : 16 * g + 16, :] = jnp.where(high_y, lower, upper)
    quarter = lane // 32
    state_a, state_b = state_ref[0:HALF, :], state_ref[HALF:MEM, :]
    column_a, column_b = column_ref[0:HALF, :], column_ref[HALF:MEM, :]
    turned = pltpu.roll(column_a, 64, 1)

    def pack(order, blocks):
        out = blocks[3]
        for n in range(3):
            out = jnp.where(quarter == order[n], blocks[n], out)
        return out

    right = pack(
        (3, 2, 1), (state_a, pltpu.roll(state_b, 96, 1), turned, pltpu.roll(column_b, 32, 1))
    )
    left = pack(
        (0, 1, 2), (state_a, pltpu.roll(state_b, 32, 1), turned, pltpu.roll(column_b, 96, 1))
    )
    near_out_ref[0:HALF, :] = jnp.where(even("gx"), right, left)
    far_out_ref[0:HALF, :] = jnp.where(even("gx"), left, right)
    records = pack(
        (0, 1, 2),
        (
            meta_ref[...],
            pltpu.roll(before[16:24], 32, 1),
            pltpu.roll(after[16:24], 64, 1),
            jnp.zeros((8, CELLS), f32),
        ),
    )
    near_out_ref[HALF : HALF + 8, :] = records
    far_out_ref[HALF : HALF + 8, :] = records


def turned_up(a, b):
    return jnp.where(lanes() % AY == 15, pltpu.roll(b, 15, 1), pltpu.roll(a, 127, 1))


def turned_down(a, b):
    return jnp.where(lanes() % AY == 0, pltpu.roll(b, 113, 1), pltpu.roll(a, 1, 1))


def turned_right(a, b):
    return pltpu.roll(jnp.where(lanes() < AY, b, a), 112, 1)


def turned_left(a, b):
    return pltpu.roll(jnp.where(lanes() >= CELLS - AY, b, a), 16, 1)


def shifted_rows(blocks):
    m0, m1, h0, h1 = blocks
    return {
        0: blocks,
        1: [turned_up(m0, h0), turned_up(m1, h1), turned_up(h0, m0), turned_up(h1, m1)],
        -1: [turned_down(m0, h0), turned_down(m1, h1), turned_down(h0, m0), turned_down(h1, m1)],
    }


def views_of(rows, count=4):
    out = {}
    for dy, blocks in rows.items():
        out[0, dy] = list(blocks[:count])
        for dx, turn in ((1, turned_right), (-1, turned_left)):
            out[dx, dy] = [turn(blocks[n], blocks[n ^ 1]) for n in range(count)]
    return out


def own_rows(blocks):
    m0, m1, h0, h1 = blocks
    return {
        0: [m0, m1],
        1: [turned_up(m0, h0), turned_up(m1, h1)],
        -1: [turned_down(m0, h0), turned_down(m1, h1)],
    }


def own_views(blocks):
    return {key: value[0] for key, value in views_of(own_rows(blocks), 1).items()}


ROWS = MEM // 8


def group(r):
    return pl.ds(pl.multiple_of(r * 8, 8), 8)


def total(block):
    return jnp.sum(block, axis=0, keepdims=True)


def spread(rows):
    return [jnp.broadcast_to(row, (8, CELLS)) for row in rows]


def scale(key):
    return TAPER[key[0] ** 2 + key[1] ** 2] / (MEM - 1)


def present():
    at_x, at_y = lax.axis_index("gx"), lax.axis_index("gy")
    return [
        flag.astype(jnp.int32)
        for flag in (
            at_x > 0,
            at_x < lax.axis_size("gx") - 1,
            at_y > 0,
            at_y < lax.axis_size("gy") - 1,
        )
    ]


def cell_weights(record, there, batch, square, mean):
    variance = square / (MEM - 1)
    pulls = damped = jnp.zeros((8, CELLS), f32)
    for g in range(batch * OB // 8, (batch + 1) * OB // 8):
        here = (record(RECORD * g) == lanes().astype(f32)) & there
        error = record(RECORD * g + 2)
        denominator = variance + error
        pull = (record(RECORD * g + 1) - mean) / denominator
        damp = 1.0 / (denominator + jnp.sqrt(error * denominator))
        pulls = pulls + jnp.where(here, pull, 0.0)
        damped = damped + jnp.where(here, damp, 0.0)
    return total(pulls), total(damped)


def column_of(records):
    return lambda at: jnp.broadcast_to(records[:, at : at + 1], (8, CELLS))


def window_kernel(
    meta_ref, state_ref, column_ref, near_ref, far_ref, anom_ref,
    field_ref, turned_ref, rows_ref, partial_ref, view_ref,
):
    lane = lanes()
    high_y = lane % AY >= 8
    before, after = sides(near_ref, far_ref, "gy")
    lower, upper = column_of(before[16:24]), column_of(after[16:24])
    _, _, has_before, has_after = present()
    records = (
        column_of(meta_ref[...]),
        lambda at: jnp.where(high_y, lower(at), upper(at)),
    )
    there = (lane >= 0, jnp.where(high_y, has_before, has_after) > 0)
    for block, ref in enumerate((state_ref, column_ref)):
        state = ref[...]
        mean = total(state) / MEM
        anom = state - mean
        field_ref[block] = anom
        square = total(anom * anom)
        pulls, damped = cell_weights(records[block], there[block], 0, square, mean)
        rows_ref[block : block + 1, :] = mean
        rows_ref[2 + block : 3 + block, :] = pulls
        rows_ref[4 + block : 5 + block, :] = damped

    for r in range(ROWS):
        at = slice(8 * r, 8 * r + 8)
        own, beside = field_ref[0, at, :], field_ref[1, at, :]
        up, down = turned_up(own, beside), turned_down(own, beside)
        turned_ref[0, 0, at, :] = up
        turned_ref[0, 1, at, :] = turned_up(beside, own)
        turned_ref[1, 0, at, :] = down
        turned_ref[1, 1, at, :] = turned_down(beside, own)
        rows = {0: own, 1: up, -1: down}
        for n, (dx, dy) in enumerate(OFFSETS):
            view = rows[dy]
            if dx == 1:
                view = turned_right(view, 0.0)
            if dx == -1:
                view = turned_left(view, 0.0)
            view_ref[n, at, :] = view

    zero = jnp.zeros((8, CELLS), f32)
    partial_ref[...] = jnp.zeros_like(partial_ref)

    def sums_of(blocks):
        sums = [[zero] * 9 for _ in blocks]
        for r in range(ROWS):
            at = slice(8 * r, 8 * r + 8)
            shifted = [view_ref[n, at, :] for n in range(9)]
            for i, block in enumerate(blocks):
                rows = block(at)
                sums[i] = [s + rows * w for s, w in zip(sums[i], shifted)]
        return sums

    (sums,) = sums_of([lambda at: field_ref[0, at, :]])
    for n in range(9):
        partial_ref[FIELDS, n : n + 1, :] = total(sums[n])

    def pair(g, carry):
        sums = sums_of([lambda at, v=2 * g + i: anom_ref[v, at, :] for i in range(2)])
        for i in range(2):
            for n in range(9):
                partial_ref[2 * g + i, n : n + 1, :] = total(sums[i][n])
        return carry

    lax.fori_loop(0, FIELDS // 2, pair, 0)


def analysis_kernel(
    meta_ref, near_y_ref, far_y_ref, near_x_ref, far_x_ref, field_ref, turned_ref, rows_ref,
    partial_ref, mean_ref, anom_ref, post_mean_hbm, post_anom_hbm,
    other_ref, moved_ref, first_ref, edge_ref, second_ref, out_ref, out_mean_ref, sem_ref,
):
    lane = lanes()
    low_x = lane < 64
    high_y = lane % AY >= 8
    has_west, has_east, has_before, has_after = present()
    before, after = sides(near_y_ref, far_y_ref, "gy")
    west, east = sides(near_x_ref, far_x_ref, "gx")
    west_column, east_column = column_of(west[HALF:]), column_of(east[HALF:])
    lower, upper = column_of(before[16:24]), column_of(after[16:24])
    records = (
        column_of(meta_ref[...]),
        lambda at: jnp.where(low_x, east_column(at), west_column(at)),
        lambda at: jnp.where(high_y, lower(at), upper(at)),
        lambda at: jnp.where(
            low_x,
            jnp.where(high_y, east_column(32 + at), east_column(64 + at)),
            jnp.where(high_y, west_column(32 + at), west_column(64 + at)),
        ),
    )
    side_x = jnp.where(low_x, has_east, has_west)
    side_y = jnp.where(high_y, has_before, has_after)
    there = (lane >= 0, side_x > 0, side_y > 0, side_x * side_y > 0)

    means = [rows_ref[0:1, :], None, rows_ref[1:2, :], None]
    pulls = [rows_ref[2:3, :], None, rows_ref[3:4, :], None]
    damped = [rows_ref[4:5, :], None, rows_ref[5:6, :], None]
    west_half, east_half = west[0:HALF], east[0:HALF]
    halves = {
        1: (
            jnp.where(low_x, east_half, west_half),
            jnp.where(low_x, pltpu.roll(east_half, 96, 1), pltpu.roll(west_half, 32, 1)),
        ),
        3: (
            pltpu.roll(jnp.where(low_x, west_half, east_half), 64, 1),
            jnp.where(low_x, pltpu.roll(east_half, 32, 1), pltpu.roll(west_half, 96, 1)),
        ),
    }
    for block, (first, second) in halves.items():
        mean = (total(first) + total(second)) / MEM
        first, second = first - mean, second - mean
        other_ref[block // 2, 0:HALF, :] = first
        other_ref[block // 2, HALF:MEM, :] = second
        square = total(first * first) + total(second * second)
        means[block] = mean
        pulls[block], damped[block] = cell_weights(records[block], there[block], 0, square, mean)

    zero = jnp.zeros((8, CELLS), f32)
    pull_views = views_of(shifted_rows(spread(pulls)))
    damp_views = views_of(shifted_rows(spread(damped)))
    edges = [(1, dy) for dy in (-1, 0, 1)]

    def at_edge(right, left):
        return jnp.where(lane >= CELLS - AY, right, jnp.where(lane < AY, left, 0.0))

    def shift_first(r, sums):
        at = group(r)
        m0, h0 = field_ref[0, at, :], field_ref[1, at, :]
        m1, h1 = other_ref[0, at, :], other_ref[1, at, :]
        rows = {
            0: [m0, m1, h0, h1],
            1: [turned_ref[0, 0, at, :], turned_up(m1, h1), turned_ref[0, 1, at, :], turned_up(h1, m1)],
            -1: [
                turned_ref[1, 0, at, :], turned_down(m1, h1), turned_ref[1, 1, at, :], turned_down(h1, m1),
            ],
        }
        shifted = views_of(rows)
        out = []
        for n, key in enumerate(OFFSETS):
            for block in range(4):
                first_ref[block, n, at, :] = shifted[key][block]
        for n, key in enumerate(OFFSETS):
            for block in range(1, 4):
                out.append(sums[n * 3 + block - 1] + shifted[key][block] * rows[0][block])
        for n, (_, dy) in enumerate(edges):
            edge = at_edge(shifted[1, dy][0], shifted[-1, dy][0])
            edge_ref[n, at, :] = edge
            out.append(sums[27 + n] + edge * m0)
        return tuple(out)

    sums = lax.fori_loop(0, ROWS, shift_first, (zero,) * 30, unroll=5)

    def completed(v, extra):
        out = {}
        for n, key in enumerate(OFFSETS):
            covariance = partial_ref[v, n : n + 1, :]
            if key[0]:
                more = total(extra[key[1] + 1])
                covariance = covariance + jnp.where(
                    lane >= CELLS - AY if key[0] == 1 else lane < AY, more, 0.0
                )
            out[key] = covariance * scale(key)
        return out

    next_means, next_squares = [], []
    for block in range(4):
        if block == 0:
            covariances = completed(FIELDS, sums[27:30])
        else:
            covariances = {
                key: total(sums[n * 3 + block - 1]) * scale(key) for n, key in enumerate(OFFSETS)
            }
        step = jnp.zeros_like(means[block])
        gains = []
        for key in OFFSETS:
            step = step + covariances[key] * pull_views[key][block][0:1]
            gains.append(covariances[key] * damp_views[key][block][0:1])
        square = zero
        for r in range(ROWS):
            at = slice(8 * r, 8 * r + 8)
            source = other_ref if block % 2 else field_ref
            moved = source[block // 2, at, :]
            for n in range(9):
                moved = moved - gains[n] * first_ref[block, n, at, :]
            moved_ref[block, at, :] = moved
            square = square + moved * moved
        next_means.append(means[block] + step)
        next_squares.append(total(square))
    next_pulls, next_damped = [], []
    for block in range(4):
        pull, damp = cell_weights(
            records[block], there[block], 1, next_squares[block], next_means[block]
        )
        next_pulls.append(pull)
        next_damped.append(damp)
    next_pull_views = own_views(spread(next_pulls))
    next_damp_views = own_views(spread(next_damped))

    def shift_second(r, sums):
        at = group(r)
        blocks = [moved_ref[block, at, :] for block in range(4)]
        shifted = own_views(blocks)
        out = []
        for n, key in enumerate(OFFSETS):
            second_ref[n, at, :] = shifted[key]
            out.append(sums[n] + shifted[key] * blocks[0])
        return tuple(out)

    sums = lax.fori_loop(0, ROWS, shift_second, (zero,) * 9, unroll=5)

    def finish(sums, mean):
        gains = []
        for n, key in enumerate(OFFSETS):
            covariance = total(sums[n]) * scale(key)
            mean = mean + covariance * next_pull_views[key][0:1]
            gains.append(covariance * next_damp_views[key][0:1])
        return gains, mean

    gains, mean = finish(sums, next_means[0])
    out_mean_ref[FIELDS] = mean
    for r in range(ROWS):
        at = slice(8 * r, 8 * r + 8)
        block = moved_ref[0, at, :]
        for n in range(9):
            block = block - gains[n] * second_ref[n, at, :]
        out_ref[FIELDS, at, :] = block

    def send(v, count):
        return pltpu.make_async_copy(
            out_ref.at[pl.ds(v, count)], post_anom_hbm.at[pl.ds(v, count)], sem_ref.at[0]
        )

    def pair(g, carry):
        comps = [2 * g, 2 * g + 1]
        sums = [[zero] * 3, [zero] * 3]
        for r in range(ROWS):
            at = slice(8 * r, 8 * r + 8)
            shifted = [edge_ref[n, at, :] for n in range(3)]
            for i, v in enumerate(comps):
                block = anom_ref[v, at, :]
                sums[i] = [s + block * w for s, w in zip(sums[i], shifted)]
        means, gains = [], []
        for i, v in enumerate(comps):
            mean = mean_ref[pl.ds(v, 1), :]
            own = []
            for key, covariance in completed(v, sums[i]).items():
                mean = mean + covariance * pull_views[key][0][0:1]
                own.append(covariance * damp_views[key][0][0:1])
            means.append(mean)
            gains.append(own)
        sums = [[zero] * 9, [zero] * 9]
        for r in range(ROWS):
            at = slice(8 * r, 8 * r + 8)
            shifted = [first_ref[0, n, at, :] for n in range(9)]
            later = [second_ref[n, at, :] for n in range(9)]
            for i, v in enumerate(comps):
                block = anom_ref[v, at, :]
                for n in range(9):
                    block = block - gains[i][n] * shifted[n]
                out_ref[v, at, :] = block
                sums[i] = [s + block * w for s, w in zip(sums[i], later)]
        for i, v in enumerate(comps):
            gains[i], mean = finish(sums[i], means[i])
            out_mean_ref[v] = mean
        for r in range(ROWS):
            at = slice(8 * r, 8 * r + 8)
            later = [second_ref[n, at, :] for n in range(9)]
            for i, v in enumerate(comps):
                block = out_ref[v, at, :]
                for n in range(9):
                    block = block - gains[i][n] * later[n]
                out_ref[v, at, :] = block
        send(2 * g, 2).start()
        return carry

    send(FIELDS, 1).start()
    lax.fori_loop(0, FIELDS // 2, pair, 0)
    last = pltpu.make_async_copy(out_mean_ref, post_mean_hbm, sem_ref.at[1])
    last.start()
    pltpu.make_async_copy(out_ref, post_anom_hbm, sem_ref.at[0]).wait()
    last.wait()


VMEM = pl.BlockSpec(memory_space=pltpu.VMEM)
SMEM = pl.BlockSpec(memory_space=pltpu.SMEM)
ANY = pl.BlockSpec(memory_space=pl.ANY)
LIMIT = pltpu.CompilerParams(vmem_limit_bytes=8 << 20)


def flat(*shape):
    return jax.ShapeDtypeStruct(shape, f32)


def local(
    atm_members,
    ocean_members,
    remap_weights,
    pair_src,
    obs_cell,
    obs_value,
    obs_error,
    obs_live,
    obs_order,
):
    at_x = lax.axis_index("gx")
    at_y = lax.axis_index("gy")
    rows = lax.axis_size("gy")
    own = ocean_members[0, 0]
    column = [own]
    for first in (0, 1):
        column.append(exchange(own, "gy", first))
    tiles = list(column)
    for first in (0, 1):
        for tile in column:
            tiles.append(exchange(tile, "gx", first))
    source = pair_src[0, 0]

    def slot(step, at):
        return jnp.where(step == 0, 0, jnp.where((step == 1) == (at % 2 == 0), 1, 2))

    select = slot(source // rows - at_x, at_x) * 3 + slot(source % rows - at_y, at_y)
    listed = select[None, :] == jnp.arange(9, dtype=jnp.int32)[:, None]
    slots = jnp.max(jnp.where(listed, jnp.arange(K, dtype=jnp.int32)[None, :], -1), axis=1)
    weights = remap_weights[0, 0]
    cell = jnp.where(obs_live[0] > 0, obs_cell[0], -1)
    slot_rows = jnp.concatenate(
        [obs_order[0].astype(f32), cell.astype(f32), obs_value[0], obs_error[0]], axis=0
    )
    meta = pl.pallas_call(
        records_kernel,
        in_specs=[ANY, VMEM],
        out_specs=VMEM,
        cost_estimate=pl.CostEstimate(flops=500000000, bytes_accessed=1000000, transcendentals=0),
        out_shape=flat(8, CELLS),
        name="records",
        compiler_params=LIMIT,
    )(column[2], slot_rows)
    early = pl.pallas_call(
        early_kernel,
        in_specs=[SMEM, ANY, VMEM] + [VMEM] * len(EARLY),
        out_specs=VMEM,
        out_shape=flat(MEM, CELLS),
        name="early",
        compiler_params=LIMIT,
    )(slots, meta, weights, *[tiles[n] for n in EARLY])
    state, near_message, far_message = pl.pallas_call(
        remap_kernel,
        in_specs=[SMEM, VMEM, VMEM, VMEM] + [VMEM] * len(LATE),
        out_specs=[VMEM] * 3,
        out_shape=[flat(MEM, CELLS), flat(24, CELLS), flat(24, CELLS)],
        name="remap",
        compiler_params=LIMIT,
    )(slots, meta, weights, early, *[tiles[n] for n in LATE])
    near_y = exchange(near_message, "gy", 0)
    far_y = exchange(far_message, "gy", 1)
    anomaly, mean = pl.pallas_call(
        fields_kernel,
        in_specs=[ANY, VMEM],
        out_specs=[VMEM, VMEM],
        out_shape=[flat(FIELDS, MEM, CELLS), flat(16, CELLS)],
        name="fields",
        compiler_params=LIMIT,
    )(state, jnp.transpose(atm_members[0, 0], (1, 0, 2)))
    beside, near_out, far_out = pl.pallas_call(
        side_kernel,
        in_specs=[VMEM] * 4,
        out_specs=[VMEM] * 3,
        out_shape=[flat(MEM, CELLS), flat(HALF + 8, CELLS), flat(HALF + 8, CELLS)],
        name="side",
        compiler_params=LIMIT,
    )(meta, state, near_y, far_y)
    near_x = exchange(near_out, "gx", 0)
    far_x = exchange(far_out, "gx", 1)
    field, turned, rows, partial = pl.pallas_call(
        window_kernel,
        in_specs=[VMEM] * 6,
        out_specs=[VMEM] * 4,
        out_shape=[
            flat(2, MEM, CELLS),
            flat(2, 2, MEM, CELLS),
            flat(8, CELLS),
            flat(COMP, 16, CELLS),
        ],
        scratch_shapes=[pltpu.VMEM((9, MEM, CELLS), f32)],
        name="window",
        compiler_params=LIMIT,
    )(meta, state, beside, near_y, far_y, anomaly)
    post_mean, post_anom = pl.pallas_call(
        analysis_kernel,
        in_specs=[VMEM] * 11,
        out_specs=[ANY, ANY],
        out_shape=[flat(COMP, 1, CELLS), flat(COMP, MEM, CELLS)],
        scratch_shapes=[
            pltpu.VMEM((2, MEM, CELLS), f32),
            pltpu.VMEM((4, MEM, CELLS), f32),
            pltpu.VMEM((4, 9, MEM, CELLS), f32),
            pltpu.VMEM((3, MEM, CELLS), f32),
            pltpu.VMEM((9, MEM, CELLS), f32),
            pltpu.VMEM((COMP, MEM, CELLS), f32),
            pltpu.VMEM((COMP, 1, CELLS), f32),
            pltpu.SemaphoreType.DMA((2,)),
        ],
        name="analysis",
        compiler_params=LIMIT,
    )(meta, near_y, far_y, near_x, far_x, field, turned, rows, partial, mean, anomaly)
    post_mean = jnp.transpose(post_mean, (1, 0, 2))
    post_anom = jnp.transpose(post_anom, (1, 0, 2))
    return post_mean[None], post_anom[None, None]


def solution(mesh):
    in_specs = (
        P("gx", "gy", None, None, None),
        P("gx", "gy", None, None),
        P("gx", "gy", None, None, None),
        P("gx", "gy", None),
        P("gx", "gy", None),
        P("gx", "gy", None),
        P("gx", "gy", None),
        P("gx", "gy", None),
        P("gx", "gy", None),
    )
    out_specs = (P("gx", "gy", None, None), P("gx", "gy", None, None, None))

    return jax.shard_map(local, mesh=mesh, in_specs=in_specs, out_specs=out_specs, check_vma=False)
```

```python
import jax
import jax.numpy as jnp
from jax import lax
from jax.experimental import pallas as pl
from jax.experimental.pallas import tpu as pltpu
from jax.sharding import PartitionSpec as P


MEM = 80
AY = 16
OB = 32
K = 4
FIELDS = 12
COMP = 13
CELLS = 128
OBS_DEV = 64

f32 = jnp.float32
RECORD = 3
TAPER = {0: 1.0, 1: 0.5625, 2: 0.25}
OFFSETS = [(dx, dy) for dx in (-1, 0, 1) for dy in (-1, 0, 1)]


def exchange(block, axis, first):
    count_x, count_y = lax.axis_size("gx"), lax.axis_size("gy")
    pairs = []
    for x in range(count_x):
        for y in range(count_y):
            at, count = (x, count_x) if axis == "gx" else (y, count_y)
            other = at ^ 1 if first == 0 else at - 1 + 2 * (at % 2)
            if not 0 <= other < count:
                to = (x, y ^ 1) if axis == "gx" else (x ^ 1, y)
            else:
                to = (other, y) if axis == "gx" else (x, other)
            pairs.append((x * count_y + y, to[0] * count_y + to[1]))
    return lax.ppermute(block, ("gx", "gy"), pairs)


def lanes(rows=1):
    return lax.broadcasted_iota(jnp.int32, (rows, CELLS), 1)


def records_kernel(first_hbm, slots_ref, meta_ref):
    order = jnp.transpose(jnp.broadcast_to(slots_ref[0:1, :], (OBS_DEV, OBS_DEV)))
    taken = order == lax.broadcasted_iota(jnp.int32, (OBS_DEV, OBS_DEV), 1).astype(f32)
    lane = lanes(8)
    records = jnp.zeros((8, CELLS), f32)
    for n in range(RECORD):
        row = slots_ref[n + 1 : n + 2, :]
        picked = jnp.sum(jnp.where(taken, row, 0.0), axis=1, keepdims=True)
        for g in range(OBS_DEV // 8):
            column = jnp.broadcast_to(picked[8 * g : 8 * g + 8], (8, CELLS))
            records = jnp.where(lane == RECORD * g + n, column, records)
    meta_ref[...] = records


def fields_kernel(state_hbm, atm_ref, anom_ref, mean_ref):
    mean_ref[...] = jnp.zeros_like(mean_ref)
    for v in range(FIELDS):
        field = atm_ref[v]
        mean = jnp.sum(field, axis=0, keepdims=True) / MEM
        mean_ref[v : v + 1, :] = mean
        anom_ref[v] = field - mean


def even(axis):
    return lax.axis_index(axis) % 2 == 0


def add_tiles(slot_ref, w_ref, indices, tiles, sum_ref):
    for index, tile in zip(indices, tiles):
        k = slot_ref[index]

        @pl.when(k >= 0)
        def _(tile=tile, k=k):
            sum_ref[...] += jnp.dot(tile[...], w_ref[k], preferred_element_type=f32)


EARLY = (0, 1, 2, 3, 6)
LATE = (4, 5, 7, 8)


def early_kernel(slot_ref, after_hbm, w_ref, *refs):
    tiles, sum_ref = refs[:-1], refs[-1]
    sum_ref[...] = jnp.zeros_like(sum_ref)
    add_tiles(slot_ref, w_ref, EARLY, tiles, sum_ref)


def remap_kernel(slot_ref, meta_ref, w_ref, sum_ref, *refs):
    tiles, (state_ref, near_ref, far_ref) = refs[:4], refs[4:]
    state_ref[...] = sum_ref[...]
    add_tiles(slot_ref, w_ref, LATE, tiles, state_ref)

    y = lanes() % AY
    high = low = jnp.zeros((16, CELLS), f32)
    for g in range(MEM // 16):
        part = state_ref[16 * g : 16 * g + 16, :]
        up = pltpu.roll(part, (CELLS - 2 * g) % CELLS, 1) if g else part
        down = pltpu.roll(part, 2 * g, 1) if g else part
        high = jnp.where(y // 2 == 7 - g, up, high)
        low = jnp.where(y // 2 == g, down, low)
    near_ref[0:16, :] = jnp.where(even("gy"), high, low)
    far_ref[0:16, :] = jnp.where(even("gy"), low, high)
    near_ref[16:24, :] = meta_ref[...]
    far_ref[16:24, :] = meta_ref[...]


def sides(near_ref, far_ref, axis):
    near, far = near_ref[...], far_ref[...]
    return jnp.where(even(axis), far, near), jnp.where(even(axis), near, far)


HALF = MEM // 2


def side_kernel(meta_ref, state_ref, near_ref, far_ref, column_ref, near_out_ref, far_out_ref):
    lane = lanes()
    before, after = sides(near_ref, far_ref, "gy")
    high_y = lane % AY >= 8
    for g in range(MEM // 16):
        lower, upper = before[0:16], after[0:16]
        if g:
            lower = pltpu.roll(lower, 2 * g, 1)
            upper = pltpu.roll(upper, CELLS - 2 * g, 1)
        column_ref[16 * g : 16 * g + 16, :] = jnp.where(high_y, lower, upper)
    quarter = lane // 32
    state_a, state_b = state_ref[0:HALF, :], state_ref[HALF:MEM, :]
    column_a, column_b = column_ref[0:HALF, :], column_ref[HALF:MEM, :]
    turned = pltpu.roll(column_a, 64, 1)

    def pack(order, blocks):
        out = blocks[3]
        for n in range(3):
            out = jnp.where(quarter == order[n], blocks[n], out)
        return out

    right = pack(
        (3, 2, 1), (state_a, pltpu.roll(state_b, 96, 1), turned, pltpu.roll(column_b, 32, 1))
    )
    left = pack(
        (0, 1, 2), (state_a, pltpu.roll(state_b, 32, 1), turned, pltpu.roll(column_b, 96, 1))
    )
    near_out_ref[0:HALF, :] = jnp.where(even("gx"), right, left)
    far_out_ref[0:HALF, :] = jnp.where(even("gx"), left, right)
    records = pack(
        (0, 1, 2),
        (
            meta_ref[...],
            pltpu.roll(before[16:24], 32, 1),
            pltpu.roll(after[16:24], 64, 1),
            jnp.zeros((8, CELLS), f32),
        ),
    )
    near_out_ref[HALF : HALF + 8, :] = records
    far_out_ref[HALF : HALF + 8, :] = records


def turned_up(a, b):
    return jnp.where(lanes() % AY == 15, pltpu.roll(b, 15, 1), pltpu.roll(a, 127, 1))


def turned_down(a, b):
    return jnp.where(lanes() % AY == 0, pltpu.roll(b, 113, 1), pltpu.roll(a, 1, 1))


def turned_right(a, b):
    return pltpu.roll(jnp.where(lanes() < AY, b, a), 112, 1)


def turned_left(a, b):
    return pltpu.roll(jnp.where(lanes() >= CELLS - AY, b, a), 16, 1)


def shifted_rows(blocks):
    m0, m1, h0, h1 = blocks
    return {
        0: blocks,
        1: [turned_up(m0, h0), turned_up(m1, h1), turned_up(h0, m0), turned_up(h1, m1)],
        -1: [turned_down(m0, h0), turned_down(m1, h1), turned_down(h0, m0), turned_down(h1, m1)],
    }


def views_of(rows, count=4):
    out = {}
    for dy, blocks in rows.items():
        out[0, dy] = list(blocks[:count])
        for dx, turn in ((1, turned_right), (-1, turned_left)):
            out[dx, dy] = [turn(blocks[n], blocks[n ^ 1]) for n in range(count)]
    return out


def own_rows(blocks):
    m0, m1, h0, h1 = blocks
    return {
        0: [m0, m1],
        1: [turned_up(m0, h0), turned_up(m1, h1)],
        -1: [turned_down(m0, h0), turned_down(m1, h1)],
    }


def own_views(blocks):
    return {key: value[0] for key, value in views_of(own_rows(blocks), 1).items()}


ROWS = MEM // 8


def group(r):
    return pl.ds(pl.multiple_of(r * 8, 8), 8)


def total(block):
    return jnp.sum(block, axis=0, keepdims=True)


def spread(rows):
    return [jnp.broadcast_to(row, (8, CELLS)) for row in rows]


def scale(key):
    return TAPER[key[0] ** 2 + key[1] ** 2] / (MEM - 1)


def present():
    at_x, at_y = lax.axis_index("gx"), lax.axis_index("gy")
    return [
        flag.astype(jnp.int32)
        for flag in (
            at_x > 0,
            at_x < lax.axis_size("gx") - 1,
            at_y > 0,
            at_y < lax.axis_size("gy") - 1,
        )
    ]


def cell_weights(record, there, batch, square, mean):
    variance = square / (MEM - 1)
    pulls = damped = jnp.zeros((8, CELLS), f32)
    for g in range(batch * OB // 8, (batch + 1) * OB // 8):
        here = (record(RECORD * g) == lanes().astype(f32)) & there
        error = record(RECORD * g + 2)
        denominator = variance + error
        pull = (record(RECORD * g + 1) - mean) / denominator
        damp = 1.0 / (denominator + jnp.sqrt(error * denominator))
        pulls = pulls + jnp.where(here, pull, 0.0)
        damped = damped + jnp.where(here, damp, 0.0)
    return total(pulls), total(damped)


def column_of(records):
    return lambda at: jnp.broadcast_to(records[:, at : at + 1], (8, CELLS))


def lanes_of(records, start):
    start = jnp.broadcast_to(start, (8, CELLS))
    return lambda at: jnp.take_along_axis(records, start + at, axis=1)


def window_kernel(
    meta_ref, state_ref, column_ref, near_ref, far_ref, anom_ref,
    field_ref, turned_ref, rows_ref, partial_ref, view_ref,
):
    lane = lanes()
    high_y = lane % AY >= 8
    before, after = sides(near_ref, far_ref, "gy")
    lower, upper = column_of(before[16:24]), column_of(after[16:24])
    _, _, has_before, has_after = present()
    records = (
        column_of(meta_ref[...]),
        lambda at: jnp.where(high_y, lower(at), upper(at)),
    )
    there = (lane >= 0, jnp.where(high_y, has_before, has_after) > 0)
    for block, ref in enumerate((state_ref, column_ref)):
        state = ref[...]
        mean = total(state) / MEM
        anom = state - mean
        field_ref[block] = anom
        square = total(anom * anom)
        pulls, damped = cell_weights(records[block], there[block], 0, square, mean)
        rows_ref[block : block + 1, :] = mean
        rows_ref[2 + block : 3 + block, :] = pulls
        rows_ref[4 + block : 5 + block, :] = damped

    for r in range(ROWS):
        at = slice(8 * r, 8 * r + 8)
        own, beside = field_ref[0, at, :], field_ref[1, at, :]
        up, down = turned_up(own, beside), turned_down(own, beside)
        turned_ref[0, 0, at, :] = up
        turned_ref[0, 1, at, :] = turned_up(beside, own)
        turned_ref[1, 0, at, :] = down
        turned_ref[1, 1, at, :] = turned_down(beside, own)
        rows = {0: own, 1: up, -1: down}
        for n, (dx, dy) in enumerate(OFFSETS):
            view = rows[dy]
            if dx == 1:
                view = turned_right(view, 0.0)
            if dx == -1:
                view = turned_left(view, 0.0)
            view_ref[n, at, :] = view

    zero = jnp.zeros((8, CELLS), f32)
    partial_ref[...] = jnp.zeros_like(partial_ref)

    def sums_of(blocks):
        sums = [[zero] * 9 for _ in blocks]
        for r in range(ROWS):
            at = slice(8 * r, 8 * r + 8)
            shifted = [view_ref[n, at, :] for n in range(9)]
            for i, block in enumerate(blocks):
                rows = block(at)
                sums[i] = [s + rows * w for s, w in zip(sums[i], shifted)]
        return sums

    (sums,) = sums_of([lambda at: field_ref[0, at, :]])
    for n in range(9):
        partial_ref[FIELDS, n : n + 1, :] = total(sums[n])

    def pair(g, carry):
        sums = sums_of([lambda at, v=2 * g + i: anom_ref[v, at, :] for i in range(2)])
        for i in range(2):
            for n in range(9):
                partial_ref[2 * g + i, n : n + 1, :] = total(sums[i][n])
        return carry

    lax.fori_loop(0, FIELDS // 2, pair, 0)


def analysis_kernel(
    meta_ref, near_y_ref, far_y_ref, near_x_ref, far_x_ref, field_ref, turned_ref, rows_ref,
    partial_ref, mean_ref, anom_ref, post_mean_hbm, post_anom_hbm,
    other_ref, moved_ref, first_ref, edge_ref, second_ref, out_ref, out_mean_ref, sem_ref,
):
    lane = lanes()
    low_x = lane < 64
    high_y = lane % AY >= 8
    has_west, has_east, has_before, has_after = present()
    before, after = sides(near_y_ref, far_y_ref, "gy")
    west, east = sides(near_x_ref, far_x_ref, "gx")
    west_records, east_records = west[HALF:], east[HALF:]
    beside_x = jnp.where(low_x, east_records, pltpu.roll(west_records, 64, 1))
    beside_y = jnp.where(low_x, before[16:24], pltpu.roll(after[16:24], 64, 1))
    corners = jnp.where(
        low_x, pltpu.roll(east_records, 96, 1), pltpu.roll(west_records, 32, 1)
    )
    records = (
        column_of(meta_ref[...]),
        lanes_of(beside_x, jnp.where(low_x, 0, 64)),
        lanes_of(beside_y, jnp.where(high_y, 0, 64)),
        lanes_of(corners, jnp.where(low_x, 0, 64) + jnp.where(high_y, 0, 32)),
    )
    side_x = jnp.where(low_x, has_east, has_west)
    side_y = jnp.where(high_y, has_before, has_after)
    there = (lane >= 0, side_x > 0, side_y > 0, side_x * side_y > 0)

    means = [rows_ref[0:1, :], None, rows_ref[1:2, :], None]
    pulls = [rows_ref[2:3, :], None, rows_ref[3:4, :], None]
    damped = [rows_ref[4:5, :], None, rows_ref[5:6, :], None]
    west_half, east_half = west[0:HALF], east[0:HALF]
    halves = {
        1: (
            jnp.where(low_x, east_half, west_half),
            jnp.where(low_x, pltpu.roll(east_half, 96, 1), pltpu.roll(west_half, 32, 1)),
        ),
        3: (
            pltpu.roll(jnp.where(low_x, west_half, east_half), 64, 1),
            jnp.where(low_x, pltpu.roll(east_half, 32, 1), pltpu.roll(west_half, 96, 1)),
        ),
    }
    for block, (first, second) in halves.items():
        mean = (total(first) + total(second)) / MEM
        first, second = first - mean, second - mean
        other_ref[block // 2, 0:HALF, :] = first
        other_ref[block // 2, HALF:MEM, :] = second
        square = total(first * first) + total(second * second)
        means[block] = mean
        pulls[block], damped[block] = cell_weights(records[block], there[block], 0, square, mean)

    zero = jnp.zeros((8, CELLS), f32)
    pull_views = views_of(shifted_rows(spread(pulls)))
    damp_views = views_of(shifted_rows(spread(damped)))
    edges = [(1, dy) for dy in (-1, 0, 1)]

    def at_edge(right, left):
        return jnp.where(lane >= CELLS - AY, right, jnp.where(lane < AY, left, 0.0))

    def shift_first(r, sums):
        at = group(r)
        m0, h0 = field_ref[0, at, :], field_ref[1, at, :]
        m1, h1 = other_ref[0, at, :], other_ref[1, at, :]
        rows = {
            0: [m0, m1, h0, h1],
            1: [turned_ref[0, 0, at, :], turned_up(m1, h1), turned_ref[0, 1, at, :], turned_up(h1, m1)],
            -1: [
                turned_ref[1, 0, at, :], turned_down(m1, h1), turned_ref[1, 1, at, :], turned_down(h1, m1),
            ],
        }
        shifted = views_of(rows)
        out = []
        for n, key in enumerate(OFFSETS):
            for block in range(4):
                first_ref[block, n, at, :] = shifted[key][block]
        for n, key in enumerate(OFFSETS):
            for block in range(1, 4):
                out.append(sums[n * 3 + block - 1] + shifted[key][block] * rows[0][block])
        for n, (_, dy) in enumerate(edges):
            edge = at_edge(shifted[1, dy][0], shifted[-1, dy][0])
            edge_ref[n, at, :] = edge
            out.append(sums[27 + n] + edge * m0)
        return tuple(out)

    sums = lax.fori_loop(0, ROWS, shift_first, (zero,) * 30, unroll=5)

    def completed(v, extra):
        out = {}
        for n, key in enumerate(OFFSETS):
            covariance = partial_ref[v, n : n + 1, :]
            if key[0]:
                more = total(extra[key[1] + 1])
                covariance = covariance + jnp.where(
                    lane >= CELLS - AY if key[0] == 1 else lane < AY, more, 0.0
                )
            out[key] = covariance * scale(key)
        return out

    next_means, next_squares = [], []
    for block in range(4):
        if block == 0:
            covariances = completed(FIELDS, sums[27:30])
        else:
            covariances = {
                key: total(sums[n * 3 + block - 1]) * scale(key) for n, key in enumerate(OFFSETS)
            }
        step = jnp.zeros_like(means[block])
        gains = []
        for key in OFFSETS:
            step = step + covariances[key] * pull_views[key][block][0:1]
            gains.append(covariances[key] * damp_views[key][block][0:1])
        square = zero
        for r in range(ROWS):
            at = slice(8 * r, 8 * r + 8)
            source = other_ref if block % 2 else field_ref
            moved = source[block // 2, at, :]
            for n in range(9):
                moved = moved - gains[n] * first_ref[block, n, at, :]
            moved_ref[block, at, :] = moved
            square = square + moved * moved
        next_means.append(means[block] + step)
        next_squares.append(total(square))
    next_pulls, next_damped = [], []
    for block in range(4):
        pull, damp = cell_weights(
            records[block], there[block], 1, next_squares[block], next_means[block]
        )
        next_pulls.append(pull)
        next_damped.append(damp)
    next_pull_views = own_views(spread(next_pulls))
    next_damp_views = own_views(spread(next_damped))

    def shift_second(r, sums):
        at = group(r)
        blocks = [moved_ref[block, at, :] for block in range(4)]
        shifted = own_views(blocks)
        out = []
        for n, key in enumerate(OFFSETS):
            second_ref[n, at, :] = shifted[key]
            out.append(sums[n] + shifted[key] * blocks[0])
        return tuple(out)

    sums = lax.fori_loop(0, ROWS, shift_second, (zero,) * 9, unroll=5)

    def finish(sums, mean):
        gains = []
        for n, key in enumerate(OFFSETS):
            covariance = total(sums[n]) * scale(key)
            mean = mean + covariance * next_pull_views[key][0:1]
            gains.append(covariance * next_damp_views[key][0:1])
        return gains, mean

    gains, mean = finish(sums, next_means[0])
    out_mean_ref[FIELDS] = mean
    for r in range(ROWS):
        at = slice(8 * r, 8 * r + 8)
        block = moved_ref[0, at, :]
        for n in range(9):
            block = block - gains[n] * second_ref[n, at, :]
        out_ref[FIELDS, at, :] = block

    def send(v, count):
        return pltpu.make_async_copy(
            out_ref.at[pl.ds(v, count)], post_anom_hbm.at[pl.ds(v, count)], sem_ref.at[0]
        )

    def pair(g, carry):
        comps = [2 * g, 2 * g + 1]
        sums = [[zero] * 3, [zero] * 3]
        for r in range(ROWS):
            at = slice(8 * r, 8 * r + 8)
            shifted = [edge_ref[n, at, :] for n in range(3)]
            for i, v in enumerate(comps):
                block = anom_ref[v, at, :]
                sums[i] = [s + block * w for s, w in zip(sums[i], shifted)]
        means, gains = [], []
        for i, v in enumerate(comps):
            mean = mean_ref[pl.ds(v, 1), :]
            own = []
            for key, covariance in completed(v, sums[i]).items():
                mean = mean + covariance * pull_views[key][0][0:1]
                own.append(covariance * damp_views[key][0][0:1])
            means.append(mean)
            gains.append(own)
        sums = [[zero] * 9, [zero] * 9]
        for r in range(ROWS):
            at = slice(8 * r, 8 * r + 8)
            shifted = [first_ref[0, n, at, :] for n in range(9)]
            later = [second_ref[n, at, :] for n in range(9)]
            for i, v in enumerate(comps):
                block = anom_ref[v, at, :]
                for n in range(9):
                    block = block - gains[i][n] * shifted[n]
                out_ref[v, at, :] = block
                sums[i] = [s + block * w for s, w in zip(sums[i], later)]
        for i, v in enumerate(comps):
            gains[i], mean = finish(sums[i], means[i])
            out_mean_ref[v] = mean
        for r in range(ROWS):
            at = slice(8 * r, 8 * r + 8)
            later = [second_ref[n, at, :] for n in range(9)]
            for i, v in enumerate(comps):
                block = out_ref[v, at, :]
                for n in range(9):
                    block = block - gains[i][n] * later[n]
                out_ref[v, at, :] = block
        send(2 * g, 2).start()
        return carry

    send(FIELDS, 1).start()
    lax.fori_loop(0, FIELDS // 2, pair, 0)
    last = pltpu.make_async_copy(out_mean_ref, post_mean_hbm, sem_ref.at[1])
    last.start()
    pltpu.make_async_copy(out_ref, post_anom_hbm, sem_ref.at[0]).wait()
    last.wait()


VMEM = pl.BlockSpec(memory_space=pltpu.VMEM)
SMEM = pl.BlockSpec(memory_space=pltpu.SMEM)
ANY = pl.BlockSpec(memory_space=pl.ANY)
LIMIT = pltpu.CompilerParams(vmem_limit_bytes=8 << 20)


def flat(*shape):
    return jax.ShapeDtypeStruct(shape, f32)


def local(
    atm_members,
    ocean_members,
    remap_weights,
    pair_src,
    obs_cell,
    obs_value,
    obs_error,
    obs_live,
    obs_order,
):
    at_x = lax.axis_index("gx")
    at_y = lax.axis_index("gy")
    rows = lax.axis_size("gy")
    own = ocean_members[0, 0]
    column = [own]
    for first in (0, 1):
        column.append(exchange(own, "gy", first))
    tiles = list(column)
    for first in (0, 1):
        for tile in column:
            tiles.append(exchange(tile, "gx", first))
    source = pair_src[0, 0]

    def slot(step, at):
        return jnp.where(step == 0, 0, jnp.where((step == 1) == (at % 2 == 0), 1, 2))

    select = slot(source // rows - at_x, at_x) * 3 + slot(source % rows - at_y, at_y)
    listed = select[None, :] == jnp.arange(9, dtype=jnp.int32)[:, None]
    slots = jnp.max(jnp.where(listed, jnp.arange(K, dtype=jnp.int32)[None, :], -1), axis=1)
    weights = remap_weights[0, 0]
    cell = jnp.where(obs_live[0] > 0, obs_cell[0], -1)
    slot_rows = jnp.concatenate(
        [obs_order[0].astype(f32), cell.astype(f32), obs_value[0], obs_error[0]], axis=0
    )
    meta = pl.pallas_call(
        records_kernel,
        in_specs=[ANY, VMEM],
        out_specs=VMEM,
        cost_estimate=pl.CostEstimate(flops=500000000, bytes_accessed=1000000, transcendentals=0),
        out_shape=flat(8, CELLS),
        name="records",
        compiler_params=LIMIT,
    )(column[2], slot_rows)
    early = pl.pallas_call(
        early_kernel,
        in_specs=[SMEM, ANY, VMEM] + [VMEM] * len(EARLY),
        out_specs=VMEM,
        out_shape=flat(MEM, CELLS),
        name="early",
        compiler_params=LIMIT,
    )(slots, meta, weights, *[tiles[n] for n in EARLY])
    state, near_message, far_message = pl.pallas_call(
        remap_kernel,
        in_specs=[SMEM, VMEM, VMEM, VMEM] + [VMEM] * len(LATE),
        out_specs=[VMEM] * 3,
        out_shape=[flat(MEM, CELLS), flat(24, CELLS), flat(24, CELLS)],
        name="remap",
        compiler_params=LIMIT,
    )(slots, meta, weights, early, *[tiles[n] for n in LATE])
    near_y = exchange(near_message, "gy", 0)
    far_y = exchange(far_message, "gy", 1)
    anomaly, mean = pl.pallas_call(
        fields_kernel,
        in_specs=[ANY, VMEM],
        out_specs=[VMEM, VMEM],
        out_shape=[flat(FIELDS, MEM, CELLS), flat(16, CELLS)],
        name="fields",
        compiler_params=LIMIT,
    )(state, jnp.transpose(atm_members[0, 0], (1, 0, 2)))
    beside, near_out, far_out = pl.pallas_call(
        side_kernel,
        in_specs=[VMEM] * 4,
        out_specs=[VMEM] * 3,
        out_shape=[flat(MEM, CELLS), flat(HALF + 8, CELLS), flat(HALF + 8, CELLS)],
        name="side",
        compiler_params=LIMIT,
    )(meta, state, near_y, far_y)
    near_x = exchange(near_out, "gx", 0)
    far_x = exchange(far_out, "gx", 1)
    field, turned, rows, partial = pl.pallas_call(
        window_kernel,
        in_specs=[VMEM] * 6,
        out_specs=[VMEM] * 4,
        out_shape=[
            flat(2, MEM, CELLS),
            flat(2, 2, MEM, CELLS),
            flat(8, CELLS),
            flat(COMP, 16, CELLS),
        ],
        scratch_shapes=[pltpu.VMEM((9, MEM, CELLS), f32)],
        name="window",
        compiler_params=LIMIT,
    )(meta, state, beside, near_y, far_y, anomaly)
    post_mean, post_anom = pl.pallas_call(
        analysis_kernel,
        in_specs=[VMEM] * 11,
        out_specs=[ANY, ANY],
        out_shape=[flat(COMP, 1, CELLS), flat(COMP, MEM, CELLS)],
        scratch_shapes=[
            pltpu.VMEM((2, MEM, CELLS), f32),
            pltpu.VMEM((4, MEM, CELLS), f32),
            pltpu.VMEM((4, 9, MEM, CELLS), f32),
            pltpu.VMEM((3, MEM, CELLS), f32),
            pltpu.VMEM((9, MEM, CELLS), f32),
            pltpu.VMEM((COMP, MEM, CELLS), f32),
            pltpu.VMEM((COMP, 1, CELLS), f32),
            pltpu.SemaphoreType.DMA((2,)),
        ],
        name="analysis",
        compiler_params=LIMIT,
    )(meta, near_y, far_y, near_x, far_x, field, turned, rows, partial, mean, anomaly)
    post_mean = jnp.transpose(post_mean, (1, 0, 2))
    post_anom = jnp.transpose(post_anom, (1, 0, 2))
    return post_mean[None], post_anom[None, None]


def solution(mesh):
    in_specs = (
        P("gx", "gy", None, None, None),
        P("gx", "gy", None, None),
        P("gx", "gy", None, None, None),
        P("gx", "gy", None),
        P("gx", "gy", None),
        P("gx", "gy", None),
        P("gx", "gy", None),
        P("gx", "gy", None),
        P("gx", "gy", None),
    )
    out_specs = (P("gx", "gy", None, None), P("gx", "gy", None, None, None))

    return jax.shard_map(local, mesh=mesh, in_specs=in_specs, out_specs=out_specs, check_vma=False)
```

```python
import jax
import jax.numpy as jnp
from jax import lax
from jax.experimental import pallas as pl
from jax.experimental.pallas import tpu as pltpu
from jax.sharding import PartitionSpec as P


MEM = 80
AY = 16
OB = 32
K = 4
FIELDS = 12
COMP = 13
CELLS = 128
OBS_DEV = 64

f32 = jnp.float32
RECORD = 3
TAPER = {0: 1.0, 1: 0.5625, 2: 0.25}
OFFSETS = [(dx, dy) for dx in (-1, 0, 1) for dy in (-1, 0, 1)]


def exchange(block, axis, first):
    count_x, count_y = lax.axis_size("gx"), lax.axis_size("gy")
    pairs = []
    for x in range(count_x):
        for y in range(count_y):
            at, count = (x, count_x) if axis == "gx" else (y, count_y)
            other = at ^ 1 if first == 0 else at - 1 + 2 * (at % 2)
            if not 0 <= other < count:
                to = (x, y ^ 1) if axis == "gx" else (x ^ 1, y)
            else:
                to = (other, y) if axis == "gx" else (x, other)
            pairs.append((x * count_y + y, to[0] * count_y + to[1]))
    return lax.ppermute(block, ("gx", "gy"), pairs)


def lanes(rows=1):
    return lax.broadcasted_iota(jnp.int32, (rows, CELLS), 1)


def records_kernel(first_hbm, slots_ref, meta_ref):
    order = jnp.transpose(jnp.broadcast_to(slots_ref[0:1, :], (OBS_DEV, OBS_DEV)))
    taken = order == lax.broadcasted_iota(jnp.int32, (OBS_DEV, OBS_DEV), 1).astype(f32)
    lane = lanes(8)
    records = jnp.zeros((8, CELLS), f32)
    for n in range(RECORD):
        row = slots_ref[n + 1 : n + 2, :]
        picked = jnp.sum(jnp.where(taken, row, 0.0), axis=1, keepdims=True)
        for g in range(OBS_DEV // 8):
            column = jnp.broadcast_to(picked[8 * g : 8 * g + 8], (8, CELLS))
            records = jnp.where(lane == RECORD * g + n, column, records)
    meta_ref[...] = records


def fields_kernel(state_hbm, atm_ref, anom_ref, mean_ref):
    mean_ref[...] = jnp.zeros_like(mean_ref)
    for v in range(FIELDS):
        field = atm_ref[v]
        mean = jnp.sum(field, axis=0, keepdims=True) / MEM
        mean_ref[v : v + 1, :] = mean
        anom_ref[v] = field - mean


def even(axis):
    return lax.axis_index(axis) % 2 == 0


def add_tiles(slot_ref, w_ref, indices, tiles, sum_ref):
    for index, tile in zip(indices, tiles):
        k = slot_ref[index]

        @pl.when(k >= 0)
        def _(tile=tile, k=k):
            sum_ref[...] += jnp.dot(tile[...], w_ref[k], preferred_element_type=f32)


EARLY = (0, 1, 2, 3, 6)
LATE = (4, 5, 7, 8)


def early_kernel(slot_ref, after_hbm, w_ref, *refs):
    tiles, sum_ref = refs[:-1], refs[-1]
    sum_ref[...] = jnp.zeros_like(sum_ref)
    add_tiles(slot_ref, w_ref, EARLY, tiles, sum_ref)


def remap_kernel(slot_ref, meta_ref, w_ref, sum_ref, *refs):
    tiles, (state_ref, near_ref, far_ref) = refs[:4], refs[4:]
    state_ref[...] = sum_ref[...]
    add_tiles(slot_ref, w_ref, LATE, tiles, state_ref)

    y = lanes() % AY
    high = low = jnp.zeros((16, CELLS), f32)
    for g in range(MEM // 16):
        part = state_ref[16 * g : 16 * g + 16, :]
        up = pltpu.roll(part, (CELLS - 2 * g) % CELLS, 1) if g else part
        down = pltpu.roll(part, 2 * g, 1) if g else part
        high = jnp.where(y // 2 == 7 - g, up, high)
        low = jnp.where(y // 2 == g, down, low)
    near_ref[0:16, :] = jnp.where(even("gy"), high, low)
    far_ref[0:16, :] = jnp.where(even("gy"), low, high)
    near_ref[16:24, :] = meta_ref[...]
    far_ref[16:24, :] = meta_ref[...]


def sides(near_ref, far_ref, axis):
    near, far = near_ref[...], far_ref[...]
    return jnp.where(even(axis), far, near), jnp.where(even(axis), near, far)


HALF = MEM // 2


def side_kernel(meta_ref, state_ref, near_ref, far_ref, column_ref, near_out_ref, far_out_ref):
    lane = lanes()
    before, after = sides(near_ref, far_ref, "gy")
    high_y = lane % AY >= 8
    for g in range(MEM // 16):
        lower, upper = before[0:16], after[0:16]
        if g:
            lower = pltpu.roll(lower, 2 * g, 1)
            upper = pltpu.roll(upper, CELLS - 2 * g, 1)
        column_ref[16 * g : 16 * g + 16, :] = jnp.where(high_y, lower, upper)
    quarter = lane // 32
    state_a, state_b = state_ref[0:HALF, :], state_ref[HALF:MEM, :]
    column_a, column_b = column_ref[0:HALF, :], column_ref[HALF:MEM, :]
    turned = pltpu.roll(column_a, 64, 1)

    def pack(order, blocks):
        out = blocks[3]
        for n in range(3):
            out = jnp.where(quarter == order[n], blocks[n], out)
        return out

    right = pack(
        (3, 2, 1), (state_a, pltpu.roll(state_b, 96, 1), turned, pltpu.roll(column_b, 32, 1))
    )
    left = pack(
        (0, 1, 2), (state_a, pltpu.roll(state_b, 32, 1), turned, pltpu.roll(column_b, 96, 1))
    )
    near_out_ref[0:HALF, :] = jnp.where(even("gx"), right, left)
    far_out_ref[0:HALF, :] = jnp.where(even("gx"), left, right)
    records = pack(
        (0, 1, 2),
        (
            meta_ref[...],
            pltpu.roll(before[16:24], 32, 1),
            pltpu.roll(after[16:24], 64, 1),
            jnp.zeros((8, CELLS), f32),
        ),
    )
    near_out_ref[HALF : HALF + 8, :] = records
    far_out_ref[HALF : HALF + 8, :] = records


def turned_up(a, b):
    return jnp.where(lanes() % AY == 15, pltpu.roll(b, 15, 1), pltpu.roll(a, 127, 1))


def turned_down(a, b):
    return jnp.where(lanes() % AY == 0, pltpu.roll(b, 113, 1), pltpu.roll(a, 1, 1))


def turned_right(a, b):
    return pltpu.roll(jnp.where(lanes() < AY, b, a), 112, 1)


def turned_left(a, b):
    return pltpu.roll(jnp.where(lanes() >= CELLS - AY, b, a), 16, 1)


def shifted_rows(blocks):
    m0, m1, h0, h1 = blocks
    return {
        0: blocks,
        1: [turned_up(m0, h0), turned_up(m1, h1), turned_up(h0, m0), turned_up(h1, m1)],
        -1: [turned_down(m0, h0), turned_down(m1, h1), turned_down(h0, m0), turned_down(h1, m1)],
    }


def views_of(rows, count=4):
    out = {}
    for dy, blocks in rows.items():
        out[0, dy] = list(blocks[:count])
        for dx, turn in ((1, turned_right), (-1, turned_left)):
            out[dx, dy] = [turn(blocks[n], blocks[n ^ 1]) for n in range(count)]
    return out


def own_rows(blocks):
    m0, m1, h0, h1 = blocks
    return {
        0: [m0, m1],
        1: [turned_up(m0, h0), turned_up(m1, h1)],
        -1: [turned_down(m0, h0), turned_down(m1, h1)],
    }


def own_views(blocks):
    return {key: value[0] for key, value in views_of(own_rows(blocks), 1).items()}


ROWS = MEM // 8


def group(r):
    return pl.ds(pl.multiple_of(r * 8, 8), 8)


def total(block):
    return jnp.sum(block, axis=0, keepdims=True)


def spread(rows):
    return [jnp.broadcast_to(row, (8, CELLS)) for row in rows]


def scale(key):
    return TAPER[key[0] ** 2 + key[1] ** 2] / (MEM - 1)


def present():
    at_x, at_y = lax.axis_index("gx"), lax.axis_index("gy")
    return [
        flag.astype(jnp.int32)
        for flag in (
            at_x > 0,
            at_x < lax.axis_size("gx") - 1,
            at_y > 0,
            at_y < lax.axis_size("gy") - 1,
        )
    ]


def cell_weights(record, there, batch, square, mean):
    variance = square / (MEM - 1)
    pulls = damped = jnp.zeros((8, CELLS), f32)
    for g in range(batch * OB // 8, (batch + 1) * OB // 8):
        here = (record(RECORD * g) == lanes().astype(f32)) & there
        error = record(RECORD * g + 2)
        denominator = variance + error
        pull = (record(RECORD * g + 1) - mean) / denominator
        damp = 1.0 / (denominator + jnp.sqrt(error * denominator))
        pulls = pulls + jnp.where(here, pull, 0.0)
        damped = damped + jnp.where(here, damp, 0.0)
    return total(pulls), total(damped)


def column_of(records):
    return lambda at: jnp.broadcast_to(records[:, at : at + 1], (8, CELLS))


def lanes_of(records, start):
    start = jnp.broadcast_to(start, (8, CELLS))
    return lambda at: jnp.take_along_axis(records, start + at, axis=1)


def window_kernel(
    meta_ref, state_ref, column_ref, near_ref, far_ref, anom_ref,
    field_ref, turned_ref, rows_ref, partial_ref, view_ref,
):
    lane = lanes()
    high_y = lane % AY >= 8
    before, after = sides(near_ref, far_ref, "gy")
    lower, upper = column_of(before[16:24]), column_of(after[16:24])
    _, _, has_before, has_after = present()
    records = (
        column_of(meta_ref[...]),
        lambda at: jnp.where(high_y, lower(at), upper(at)),
    )
    there = (lane >= 0, jnp.where(high_y, has_before, has_after) > 0)
    for block, ref in enumerate((state_ref, column_ref)):
        state = ref[...]
        mean = total(state) / MEM
        anom = state - mean
        field_ref[block] = anom
        square = total(anom * anom)
        pulls, damped = cell_weights(records[block], there[block], 0, square, mean)
        rows_ref[block : block + 1, :] = mean
        rows_ref[2 + block : 3 + block, :] = pulls
        rows_ref[4 + block : 5 + block, :] = damped

    for r in range(ROWS):
        at = slice(8 * r, 8 * r + 8)
        own, beside = field_ref[0, at, :], field_ref[1, at, :]
        up, down = turned_up(own, beside), turned_down(own, beside)
        turned_ref[0, 0, at, :] = up
        turned_ref[0, 1, at, :] = turned_up(beside, own)
        turned_ref[1, 0, at, :] = down
        turned_ref[1, 1, at, :] = turned_down(beside, own)
        rows = {0: own, 1: up, -1: down}
        for n, (dx, dy) in enumerate(OFFSETS):
            view = rows[dy]
            if dx == 1:
                view = turned_right(view, 0.0)
            if dx == -1:
                view = turned_left(view, 0.0)
            view_ref[n, at, :] = view

    zero = jnp.zeros((8, CELLS), f32)
    partial_ref[...] = jnp.zeros_like(partial_ref)

    def sums_of(blocks):
        sums = [[zero] * 9 for _ in blocks]
        for r in range(ROWS):
            at = slice(8 * r, 8 * r + 8)
            shifted = [view_ref[n, at, :] for n in range(9)]
            for i, block in enumerate(blocks):
                rows = block(at)
                sums[i] = [s + rows * w for s, w in zip(sums[i], shifted)]
        return sums

    (sums,) = sums_of([lambda at: field_ref[0, at, :]])
    for n in range(9):
        partial_ref[FIELDS, n : n + 1, :] = total(sums[n])

    def pair(g, carry):
        sums = sums_of([lambda at, v=2 * g + i: anom_ref[v, at, :] for i in range(2)])
        for i in range(2):
            for n in range(9):
                partial_ref[2 * g + i, n : n + 1, :] = total(sums[i][n])
        return carry

    lax.fori_loop(0, FIELDS // 2, pair, 0)


def analysis_kernel(
    meta_ref, near_y_ref, far_y_ref, near_x_ref, far_x_ref, field_ref, turned_ref, rows_ref,
    partial_ref, mean_ref, anom_ref, post_mean_hbm, post_anom_hbm,
    other_ref, moved_ref, first_ref, edge_ref, second_ref, out_ref, out_mean_ref, sem_ref,
):
    lane = lanes()
    low_x = lane < 64
    high_y = lane % AY >= 8
    has_west, has_east, has_before, has_after = present()
    before, after = sides(near_y_ref, far_y_ref, "gy")
    west, east = sides(near_x_ref, far_x_ref, "gx")
    west_records, east_records = west[HALF:], east[HALF:]
    beside_x = jnp.where(low_x, east_records, pltpu.roll(west_records, 64, 1))
    beside_y = jnp.where(low_x, before[16:24], pltpu.roll(after[16:24], 64, 1))
    corners = jnp.where(
        low_x, pltpu.roll(east_records, 96, 1), pltpu.roll(west_records, 32, 1)
    )
    records = (
        column_of(meta_ref[...]),
        lanes_of(beside_x, jnp.where(low_x, 0, 64)),
        lanes_of(beside_y, jnp.where(high_y, 0, 64)),
        lanes_of(corners, jnp.where(low_x, 0, 64) + jnp.where(high_y, 0, 32)),
    )
    side_x = jnp.where(low_x, has_east, has_west)
    side_y = jnp.where(high_y, has_before, has_after)
    there = (lane >= 0, side_x > 0, side_y > 0, side_x * side_y > 0)

    means = [rows_ref[0:1, :], None, rows_ref[1:2, :], None]
    pulls = [rows_ref[2:3, :], None, rows_ref[3:4, :], None]
    damped = [rows_ref[4:5, :], None, rows_ref[5:6, :], None]
    west_half, east_half = west[0:HALF], east[0:HALF]
    halves = {
        1: (
            jnp.where(low_x, east_half, west_half),
            jnp.where(low_x, pltpu.roll(east_half, 96, 1), pltpu.roll(west_half, 32, 1)),
        ),
        3: (
            pltpu.roll(jnp.where(low_x, west_half, east_half), 64, 1),
            jnp.where(low_x, pltpu.roll(east_half, 32, 1), pltpu.roll(west_half, 96, 1)),
        ),
    }
    for block, (first, second) in halves.items():
        mean = (total(first) + total(second)) / MEM
        first, second = first - mean, second - mean
        other_ref[block // 2, 0:HALF, :] = first
        other_ref[block // 2, HALF:MEM, :] = second
        square = total(first * first) + total(second * second)
        means[block] = mean
        pulls[block], damped[block] = cell_weights(records[block], there[block], 0, square, mean)

    zero = jnp.zeros((8, CELLS), f32)
    pull_views = views_of(shifted_rows(spread(pulls)))
    damp_views = views_of(shifted_rows(spread(damped)))
    edges = [(1, dy) for dy in (-1, 0, 1)]

    def at_edge(right, left):
        return jnp.where(lane >= CELLS - AY, right, jnp.where(lane < AY, left, 0.0))

    def shift_first(r, sums):
        at = group(r)
        m0, h0 = field_ref[0, at, :], field_ref[1, at, :]
        m1, h1 = other_ref[0, at, :], other_ref[1, at, :]
        rows = {
            0: [m0, m1, h0, h1],
            1: [turned_ref[0, 0, at, :], turned_up(m1, h1), turned_ref[0, 1, at, :], turned_up(h1, m1)],
            -1: [
                turned_ref[1, 0, at, :], turned_down(m1, h1), turned_ref[1, 1, at, :], turned_down(h1, m1),
            ],
        }
        shifted = views_of(rows)
        out = []
        for n, key in enumerate(OFFSETS):
            for block in range(4):
                first_ref[block, n, at, :] = shifted[key][block]
        for n, key in enumerate(OFFSETS):
            for block in range(1, 4):
                out.append(sums[n * 3 + block - 1] + shifted[key][block] * rows[0][block])
        for n, (_, dy) in enumerate(edges):
            edge = at_edge(shifted[1, dy][0], shifted[-1, dy][0])
            edge_ref[n, at, :] = edge
            out.append(sums[27 + n] + edge * m0)
        return tuple(out)

    sums = lax.fori_loop(0, ROWS, shift_first, (zero,) * 30, unroll=5)

    def completed(v, extra):
        out = {}
        for n, key in enumerate(OFFSETS):
            covariance = partial_ref[v, n : n + 1, :]
            if key[0]:
                more = total(extra[key[1] + 1])
                covariance = covariance + jnp.where(
                    lane >= CELLS - AY if key[0] == 1 else lane < AY, more, 0.0
                )
            out[key] = covariance * scale(key)
        return out

    next_means, next_squares = [], []
    for block in range(4):
        if block == 0:
            covariances = completed(FIELDS, sums[27:30])
        else:
            covariances = {
                key: total(sums[n * 3 + block - 1]) * scale(key) for n, key in enumerate(OFFSETS)
            }
        step = jnp.zeros_like(means[block])
        gains = []
        for key in OFFSETS:
            step = step + covariances[key] * pull_views[key][block][0:1]
            gains.append(covariances[key] * damp_views[key][block][0:1])
        square = zero
        for r in range(ROWS):
            at = slice(8 * r, 8 * r + 8)
            source = other_ref if block % 2 else field_ref
            moved = source[block // 2, at, :]
            for n in range(9):
                moved = moved - gains[n] * first_ref[block, n, at, :]
            moved_ref[block, at, :] = moved
            square = square + moved * moved
        next_means.append(means[block] + step)
        next_squares.append(total(square))
    next_pulls, next_damped = [], []
    for block in range(4):
        pull, damp = cell_weights(
            records[block], there[block], 1, next_squares[block], next_means[block]
        )
        next_pulls.append(pull)
        next_damped.append(damp)
    next_pull_views = own_views(spread(next_pulls))
    next_damp_views = own_views(spread(next_damped))

    def shift_second(r, sums):
        at = group(r)
        blocks = [moved_ref[block, at, :] for block in range(4)]
        shifted = own_views(blocks)
        out = []
        for n, key in enumerate(OFFSETS):
            second_ref[n, at, :] = shifted[key]
            out.append(sums[n] + shifted[key] * blocks[0])
        return tuple(out)

    sums = lax.fori_loop(0, ROWS, shift_second, (zero,) * 9, unroll=5)

    def finish(sums, mean):
        gains = []
        for n, key in enumerate(OFFSETS):
            covariance = total(sums[n]) * scale(key)
            mean = mean + covariance * next_pull_views[key][0:1]
            gains.append(covariance * next_damp_views[key][0:1])
        return gains, mean

    gains, mean = finish(sums, next_means[0])
    out_mean_ref[FIELDS] = mean
    for r in range(ROWS):
        at = slice(8 * r, 8 * r + 8)
        block = moved_ref[0, at, :]
        for n in range(9):
            block = block - gains[n] * second_ref[n, at, :]
        out_ref[FIELDS, at, :] = block

    def send(v, count):
        return pltpu.make_async_copy(
            out_ref.at[pl.ds(v, count)], post_anom_hbm.at[pl.ds(v, count)], sem_ref.at[0]
        )

    def begin(g):
        comps = [g]
        sums = [[zero] * 3]
        for r in range(ROWS):
            at = slice(8 * r, 8 * r + 8)
            shifted = [edge_ref[n, at, :] for n in range(3)]
            for i, v in enumerate(comps):
                block = anom_ref[v, at, :]
                sums[i] = [s + block * w for s, w in zip(sums[i], shifted)]
        means, gains = [], []
        for i, v in enumerate(comps):
            mean = mean_ref[pl.ds(v, 1), :]
            own = []
            for key, covariance in completed(v, sums[i]).items():
                mean = mean + covariance * pull_views[key][0][0:1]
                own.append(covariance * damp_views[key][0][0:1])
            means.append(mean)
            gains.append(own)
        sums = [[zero] * 9]
        for r in range(ROWS):
            at = slice(8 * r, 8 * r + 8)
            shifted = [first_ref[0, n, at, :] for n in range(9)]
            later = [second_ref[n, at, :] for n in range(9)]
            for i, v in enumerate(comps):
                block = anom_ref[v, at, :]
                for n in range(9):
                    block = block - gains[i][n] * shifted[n]
                out_ref[v, at, :] = block
                sums[i] = [s + block * w for s, w in zip(sums[i], later)]
        return tuple(sums[0]), means[0]

    def end(g, carry):
        gains = []
        for _ in range(1):
            own, mean = finish(carry[0], carry[1])
            gains.append(own)
            out_mean_ref[g] = mean
        for r in range(ROWS):
            at = slice(8 * r, 8 * r + 8)
            later = [second_ref[n, at, :] for n in range(9)]
            for i in range(1):
                block = out_ref[g, at, :]
                for n in range(9):
                    block = block - gains[i][n] * later[n]
                out_ref[g, at, :] = block
        send(g, 1).start()

    def step(g, carry):
        end(g - 1, carry)
        return begin(g)

    send(FIELDS, 1).start()
    end(FIELDS - 1, lax.fori_loop(1, FIELDS, step, begin(0)))
    last = pltpu.make_async_copy(out_mean_ref, post_mean_hbm, sem_ref.at[1])
    last.start()
    pltpu.make_async_copy(out_ref, post_anom_hbm, sem_ref.at[0]).wait()
    last.wait()


VMEM = pl.BlockSpec(memory_space=pltpu.VMEM)
SMEM = pl.BlockSpec(memory_space=pltpu.SMEM)
ANY = pl.BlockSpec(memory_space=pl.ANY)
LIMIT = pltpu.CompilerParams(vmem_limit_bytes=8 << 20)


def flat(*shape):
    return jax.ShapeDtypeStruct(shape, f32)


def local(
    atm_members,
    ocean_members,
    remap_weights,
    pair_src,
    obs_cell,
    obs_value,
    obs_error,
    obs_live,
    obs_order,
):
    at_x = lax.axis_index("gx")
    at_y = lax.axis_index("gy")
    rows = lax.axis_size("gy")
    own = ocean_members[0, 0]
    column = [own]
    for first in (0, 1):
        column.append(exchange(own, "gy", first))
    tiles = list(column)
    for first in (0, 1):
        for tile in column:
            tiles.append(exchange(tile, "gx", first))
    source = pair_src[0, 0]

    def slot(step, at):
        return jnp.where(step == 0, 0, jnp.where((step == 1) == (at % 2 == 0), 1, 2))

    select = slot(source // rows - at_x, at_x) * 3 + slot(source % rows - at_y, at_y)
    listed = select[None, :] == jnp.arange(9, dtype=jnp.int32)[:, None]
    slots = jnp.max(jnp.where(listed, jnp.arange(K, dtype=jnp.int32)[None, :], -1), axis=1)
    weights = remap_weights[0, 0]
    cell = jnp.where(obs_live[0] > 0, obs_cell[0], -1)
    slot_rows = jnp.concatenate(
        [obs_order[0].astype(f32), cell.astype(f32), obs_value[0], obs_error[0]], axis=0
    )
    meta = pl.pallas_call(
        records_kernel,
        in_specs=[ANY, VMEM],
        out_specs=VMEM,
        cost_estimate=pl.CostEstimate(flops=500000000, bytes_accessed=1000000, transcendentals=0),
        out_shape=flat(8, CELLS),
        name="records",
        compiler_params=LIMIT,
    )(column[2], slot_rows)
    early = pl.pallas_call(
        early_kernel,
        in_specs=[SMEM, ANY, VMEM] + [VMEM] * len(EARLY),
        out_specs=VMEM,
        out_shape=flat(MEM, CELLS),
        name="early",
        compiler_params=LIMIT,
    )(slots, meta, weights, *[tiles[n] for n in EARLY])
    state, near_message, far_message = pl.pallas_call(
        remap_kernel,
        in_specs=[SMEM, VMEM, VMEM, VMEM] + [VMEM] * len(LATE),
        out_specs=[VMEM] * 3,
        out_shape=[flat(MEM, CELLS), flat(24, CELLS), flat(24, CELLS)],
        name="remap",
        compiler_params=LIMIT,
    )(slots, meta, weights, early, *[tiles[n] for n in LATE])
    near_y = exchange(near_message, "gy", 0)
    far_y = exchange(far_message, "gy", 1)
    anomaly, mean = pl.pallas_call(
        fields_kernel,
        in_specs=[ANY, VMEM],
        out_specs=[VMEM, VMEM],
        out_shape=[flat(FIELDS, MEM, CELLS), flat(16, CELLS)],
        name="fields",
        compiler_params=LIMIT,
    )(state, jnp.transpose(atm_members[0, 0], (1, 0, 2)))
    beside, near_out, far_out = pl.pallas_call(
        side_kernel,
        in_specs=[VMEM] * 4,
        out_specs=[VMEM] * 3,
        out_shape=[flat(MEM, CELLS), flat(HALF + 8, CELLS), flat(HALF + 8, CELLS)],
        name="side",
        compiler_params=LIMIT,
    )(meta, state, near_y, far_y)
    near_x = exchange(near_out, "gx", 0)
    far_x = exchange(far_out, "gx", 1)
    field, turned, rows, partial = pl.pallas_call(
        window_kernel,
        in_specs=[VMEM] * 6,
        out_specs=[VMEM] * 4,
        out_shape=[
            flat(2, MEM, CELLS),
            flat(2, 2, MEM, CELLS),
            flat(8, CELLS),
            flat(COMP, 16, CELLS),
        ],
        scratch_shapes=[pltpu.VMEM((9, MEM, CELLS), f32)],
        name="window",
        compiler_params=LIMIT,
    )(meta, state, beside, near_y, far_y, anomaly)
    post_mean, post_anom = pl.pallas_call(
        analysis_kernel,
        in_specs=[VMEM] * 11,
        out_specs=[ANY, ANY],
        out_shape=[flat(COMP, 1, CELLS), flat(COMP, MEM, CELLS)],
        scratch_shapes=[
            pltpu.VMEM((2, MEM, CELLS), f32),
            pltpu.VMEM((4, MEM, CELLS), f32),
            pltpu.VMEM((4, 9, MEM, CELLS), f32),
            pltpu.VMEM((3, MEM, CELLS), f32),
            pltpu.VMEM((9, MEM, CELLS), f32),
            pltpu.VMEM((COMP, MEM, CELLS), f32),
            pltpu.VMEM((COMP, 1, CELLS), f32),
            pltpu.SemaphoreType.DMA((2,)),
        ],
        name="analysis",
        compiler_params=LIMIT,
    )(meta, near_y, far_y, near_x, far_x, field, turned, rows, partial, mean, anomaly)
    post_mean = jnp.transpose(post_mean, (1, 0, 2))
    post_anom = jnp.transpose(post_anom, (1, 0, 2))
    return post_mean[None], post_anom[None, None]


def solution(mesh):
    in_specs = (
        P("gx", "gy", None, None, None),
        P("gx", "gy", None, None),
        P("gx", "gy", None, None, None),
        P("gx", "gy", None),
        P("gx", "gy", None),
        P("gx", "gy", None),
        P("gx", "gy", None),
        P("gx", "gy", None),
        P("gx", "gy", None),
    )
    out_specs = (P("gx", "gy", None, None), P("gx", "gy", None, None, None))

    return jax.shard_map(local, mesh=mesh, in_specs=in_specs, out_specs=out_specs, check_vma=False)
```
